8 devices in a mesh: sweep: 1 (over z), data: 2 (over y), ent: 4 (over x, core).
Axes of the slice: x: 2, y: 2, z: 1, core: 2. Of those that a mesh axis runs over, the one named last changes fastest.
Arguments:
- ent_table: float32 [16384, 512], P(('sweep', 'ent'))
- ent_state: float32 [16384], P(('sweep', 'ent'))
- rel_table: float32 [18, 512], P('sweep')
- head_idx: int32 [4, 4, 4096], P(('sweep', 'ent'), None, 'data')
- tail_idx: int32 [4, 4, 4096], P(('sweep', 'ent'), None, 'data')
- rel_idx: int32 [4, 4, 4096], P(('sweep', 'ent'), None, 'data')
- edge_mask: int32 [4, 4, 4096], P(('sweep', 'ent'), None, 'data')
- neg_idx: int32 [4, 4, 1024], P(('sweep', 'ent'))
Outputs:
- output 1: float32 [16384, 512], P(('sweep', 'ent'))
- output 2: float32 [16384], P(('sweep', 'ent'))
- output 3: float32 [18, 512], P('sweep')
- output 4: float32 [4, 4], P(('sweep', 'ent'))
All inputs are finite; a program needn't handle non-finite values.
Results may differ from the reference program's by a relative error of at most 0.001.
Values are sent between devices in bfloat16 or wider.
A program may use at most 1 GiB of HBM per device.

```python
import jax
import jax.numpy as jnp
from jax import lax

ENT_GROUP = 4
DATA_REPS = 2
ROWS_DEV = 4096
EDGES_DEV = 2048
NEG_COUNT = 1024
EMBED_DIM = 512
REL_COUNT = 18
HOT_IDS = 16

TOTAL_ROWS = ENT_GROUP * ROWS_DEV
BUCKET_EDGES = DATA_REPS * EDGES_DEV
LR_SCALE = 0.2
EPSILON = 1e-8


def draw_edges(edge_key):
    subkeys = jax.random.split(edge_key, 14)
    edge_shape = (ENT_GROUP, ENT_GROUP, BUCKET_EDGES)
    hot_ent = jax.random.randint(subkeys[0], (ENT_GROUP, HOT_IDS), 0, ROWS_DEV)
    hot_rel = jax.random.randint(subkeys[1], (HOT_IDS,), 0, REL_COUNT)
    group_ids = jnp.arange(ENT_GROUP)
    tail_group = (group_ids[:, None] + group_ids[None, :]) % ENT_GROUP
    head_hot = jnp.broadcast_to(hot_ent[:, None, :], (ENT_GROUP, ENT_GROUP, HOT_IDS))
    tail_hot = hot_ent[tail_group]

    def pick_rows(key_use, key_slot, key_uni, hot_rows):
        use_hot = jax.random.randint(key_use, edge_shape, 0, 4) == 0
        hot_slot = jax.random.randint(key_slot, edge_shape, 0, HOT_IDS)
        hot_pick = jnp.take_along_axis(hot_rows, hot_slot, axis=2)
        uni_pick = jax.random.randint(key_uni, edge_shape, 0, ROWS_DEV)
        return jnp.where(use_hot, hot_pick, uni_pick)

    head_idx = pick_rows(subkeys[2], subkeys[3], subkeys[4], head_hot)
    tail_idx = pick_rows(subkeys[5], subkeys[6], subkeys[7], tail_hot)
    rel_use = jax.random.randint(subkeys[8], edge_shape, 0, 2) == 0
    rel_slot = jax.random.randint(subkeys[9], edge_shape, 0, HOT_IDS)
    rel_uni = jax.random.randint(subkeys[10], edge_shape, 0, REL_COUNT)
    rel_idx = jnp.where(rel_use, hot_rel[rel_slot], rel_uni)
    keep_level = jax.random.randint(subkeys[11], (ENT_GROUP, ENT_GROUP, 1), 1, 17)
    edge_mask = (jax.random.randint(subkeys[12], edge_shape, 0, 16) < keep_level).astype(jnp.int32)
    neg_idx = jax.random.randint(subkeys[13], (ENT_GROUP, ENT_GROUP, NEG_COUNT), 0, ROWS_DEV)
    head_idx = head_idx.at[:, :, 0].set(ROWS_DEV - 1)
    tail_idx = tail_idx.at[:, :, 0].set(ROWS_DEV - 1)
    neg_idx = neg_idx.at[:, :, 0].set(ROWS_DEV - 1)
    rel_idx = rel_idx.at[:, :, 0].set(REL_COUNT - 1)
    return head_idx, tail_idx, rel_idx, edge_mask, neg_idx


def setup_inputs(seed: int = 0, part: int = 0) -> dict:
    part_key = jax.random.fold_in(jax.random.key(seed), part)
    subkeys = jax.random.split(part_key, 4)
    emb_scale = EMBED_DIM ** -0.25
    ent_table = jax.random.normal(subkeys[0], (TOTAL_ROWS, EMBED_DIM), jnp.float32) * emb_scale
    ent_state = jax.random.uniform(subkeys[1], (TOTAL_ROWS,), jnp.float32, 0.01, 0.1) * EMBED_DIM ** -0.5
    rel_table = jax.random.normal(subkeys[2], (REL_COUNT, EMBED_DIM), jnp.float32) * 0.7
    head_idx, tail_idx, rel_idx, edge_mask, neg_idx = draw_edges(subkeys[3])
    return {'ent_table': ent_table, 'ent_state': ent_state, 'rel_table': rel_table, 'head_idx': head_idx, 'tail_idx': tail_idx, 'rel_idx': rel_idx, 'edge_mask': edge_mask, 'neg_idx': neg_idx}


def adagrad(param_rows, accum_rows, grad_rows, learn_rate):
    accum_new = accum_rows + jnp.mean(grad_rows * grad_rows, axis=-1)
    step_rows = grad_rows / jnp.sqrt(accum_new + EPSILON)[..., None]
    return param_rows - learn_rate * step_rows, accum_new


def bucket_terms(head_rows, rel_rows, tail_bf, neg_bf, weight):
    half_dim = head_rows.shape[1] // 2
    re_h = head_rows[:, :half_dim]
    im_h = head_rows[:, half_dim:]
    re_r = rel_rows[:, :half_dim]
    im_r = rel_rows[:, half_dim:]
    query_vec = jnp.concatenate([re_h * re_r - im_h * im_r, re_h * im_r + im_h * re_r], axis=1)
    query_bf = query_vec.astype(jnp.bfloat16)
    query_wide = query_bf.astype(jnp.float32)
    tail_wide = tail_bf.astype(jnp.float32)
    pos_score = jnp.sum(query_wide * tail_wide, axis=1)
    neg_score = jnp.dot(query_bf, neg_bf.T, preferred_element_type=jnp.float32)
    top_score = jnp.maximum(jnp.max(neg_score, axis=1), pos_score)
    pos_exp = jnp.exp(pos_score - top_score)
    neg_exp = jnp.exp(neg_score - top_score[:, None])
    exp_total = pos_exp + jnp.sum(neg_exp, axis=1)
    log_total = top_score + jnp.log(exp_total)
    loss_sum = jnp.sum(weight * (log_total - pos_score))
    d_pos = weight * (pos_exp / exp_total - 1.0)
    d_neg = ((weight / exp_total)[:, None] * neg_exp).astype(jnp.bfloat16)
    grad_query = d_pos[:, None] * tail_wide + jnp.dot(d_neg, neg_bf, preferred_element_type=jnp.float32)
    grad_tail = d_pos[:, None] * query_wide
    grad_neg = jnp.dot(d_neg.T, query_bf, preferred_element_type=jnp.float32)
    re_g = grad_query[:, :half_dim]
    im_g = grad_query[:, half_dim:]
    grad_head = jnp.concatenate([re_g * re_r + im_g * im_r, im_g * re_r - re_g * im_r], axis=1)
    grad_rel = jnp.concatenate([re_g * re_h + im_g * im_h, im_g * re_h - re_g * im_h], axis=1)
    return loss_sum, grad_head, grad_rel, grad_tail, grad_neg


def reference(ent_table, ent_state, rel_table, head_idx, tail_idx, rel_idx, edge_mask, neg_idx):
    groups = head_idx.shape[0]
    part_rows = ent_table.shape[0] // groups
    emb_width = ent_table.shape[1]
    rel_rows = rel_table.shape[0]
    bucket_edges = head_idx.shape[2]
    share_edges = bucket_edges // DATA_REPS
    learn_rate = LR_SCALE * emb_width ** -0.25
    pair_ids = jnp.arange(groups * DATA_REPS)

    def one_pass(pass_carry, step_idx):
        table_now, state_now, rel_now, rel_state = pass_carry
        table_bf = table_now.astype(jnp.bfloat16)

        def one_share(grad_acc, pair_id):
            ent_grad, rel_grad = grad_acc
            group_id = pair_id // DATA_REPS
            edge_start = (pair_id % DATA_REPS) * share_edges
            tail_base = ((group_id + step_idx) % groups) * part_rows
            h_ids = lax.dynamic_slice_in_dim(head_idx[group_id, step_idx], edge_start, share_edges) + group_id * part_rows
            t_ids = lax.dynamic_slice_in_dim(tail_idx[group_id, step_idx], edge_start, share_edges) + tail_base
            r_ids = lax.dynamic_slice_in_dim(rel_idx[group_id, step_idx], edge_start, share_edges)
            weight = lax.dynamic_slice_in_dim(edge_mask[group_id, step_idx], edge_start, share_edges).astype(jnp.float32)
            n_ids = neg_idx[group_id, step_idx] + tail_base
            loss_sum, g_head, g_rel, g_tail, g_neg = bucket_terms(table_now[h_ids], rel_now[r_ids], table_bf[t_ids], table_bf[n_ids], weight)
            ent_grad = ent_grad.at[h_ids].add(g_head).at[t_ids].add(g_tail).at[n_ids].add(g_neg)
            rel_grad = rel_grad.at[r_ids].add(g_rel)
            return (ent_grad, rel_grad), loss_sum

        share_init = (jnp.zeros_like(table_now), jnp.zeros_like(rel_now))
        grads_end, share_loss = lax.scan(one_share, share_init, pair_ids)
        ent_grad, rel_grad = grads_end
        table_now, state_now = adagrad(table_now, state_now, ent_grad, learn_rate)
        rel_now, rel_state = adagrad(rel_now, rel_state, rel_grad, learn_rate)
        bucket_loss = share_loss.reshape(groups, DATA_REPS).sum(axis=1) / bucket_edges
        return (table_now, state_now, rel_now, rel_state), bucket_loss

    pass_init = (ent_table, ent_state, rel_table, jnp.zeros((rel_rows,), jnp.float32))
    pass_end, losses = lax.scan(one_pass, pass_init, jnp.arange(groups))
    return pass_end[0], pass_end[1], pass_end[2], losses.T
```

```python
import functools

import jax
import jax.numpy as jnp
from jax import lax
from jax.experimental import pallas as pl
from jax.experimental.pallas import tpu as pltpu
from jax.sharding import PartitionSpec as P

LR_SCALE = 0.2
EPSILON = 1e-8
LANES = 128
BLOCK = 512
UNROLL = 32
ACCS = 2
MIB = 2 ** 20
F32 = jnp.float32
BF16 = jnp.bfloat16


def to_flat(table):
    rows, width = table.shape
    parts = width // LANES
    return table.reshape(rows // 8, 8, parts, LANES).transpose(0, 2, 1, 3).reshape(rows * parts, LANES)


def from_flat(flat, parts):
    rows = flat.shape[0] // parts
    return flat.reshape(rows // 8, parts, 8, LANES).transpose(0, 2, 1, 3).reshape(rows, parts * LANES)


def flat_row(ids):
    return (ids >> 3) * 32 + (ids & 7)


def chunks_of(flat):
    groups = flat.shape[0] // 32
    cube = flat.reshape(groups, 32, LANES)
    return [cube[:, 8 * c : 8 * c + 8, :].reshape(groups * 8, LANES) for c in range(4)]


def flat_of(chunks):
    groups = chunks[0].shape[0] // 8
    cube = jnp.concatenate([c.reshape(groups, 8, LANES) for c in chunks], axis=1)
    return cube.reshape(groups * 32, LANES)


def split_cols(mat):
    return [mat[:, LANES * c : LANES * (c + 1)] for c in range(4)]


def split3(mat):
    hi = mat.astype(BF16)
    rest = mat - hi.astype(F32)
    mid = rest.astype(BF16)
    low = (rest - mid.astype(F32)).astype(BF16)
    return hi, mid, low


def row_at(start):
    return pl.ds(start, 4, stride=8)


def gather_rows(ids, first, count, table, out):
    def some(g, carry):
        base = g * UNROLL
        for u in range(UNROLL):
            out[row_at(base * 4 + (u // 8) * 32 + u % 8), :] = table[row_at(ids[first + base + u]), :]
        return carry

    lax.fori_loop(0, count // UNROLL, some, 0)


def head_kernel(ids, table, meta, rel3, eh_out, qb_out):
    step = pl.program_id(0)
    gather_rows(ids, step * BLOCK, BLOCK, table, eh_out)
    rr = split_cols(jnp.dot(meta[...], rel3[...], preferred_element_type=F32))
    eh = chunks_of(eh_out[...])
    q = [eh[c] * rr[c] - eh[c + 2] * rr[c + 2] for c in (0, 1)]
    q += [eh[c] * rr[c + 2] + eh[c + 2] * rr[c] for c in (0, 1)]
    qb_out[...] = jnp.concatenate(q, axis=1).astype(BF16)


def bucket_kernel(t_ids, n_ids, tail, qb, eh, meta, rel3, gh_out, gneg_out, dp_out, grel_out, loss_out, table, nb, rows_buf):
    step = pl.program_id(0)

    @pl.when(step == 0)
    def _():
        def widen(g, carry):
            table[pl.ds(pl.multiple_of(g * 512, 512), 512), :] = tail[pl.ds(pl.multiple_of(g * 512, 512), 512), :].astype(F32)
            return carry

        lax.fori_loop(0, table.shape[0] // 512, widen, 0)
        negs = nb.shape[0]
        for first in range(0, negs, BLOCK):
            gather_rows(n_ids, first, BLOCK, table, rows_buf)
            nb[first : first + BLOCK, :] = jnp.concatenate(chunks_of(rows_buf[...]), axis=1).astype(BF16)
        gneg_out[...] = jnp.zeros_like(gneg_out)
        grel_out[...] = jnp.zeros_like(grel_out)
        loss_out[...] = jnp.zeros_like(loss_out)

    gather_rows(t_ids, step * BLOCK, BLOCK, table, rows_buf)
    tb = chunks_of(rows_buf[...])
    qv = qb[...]
    qf = split_cols(qv.astype(F32))
    s = lax.dot_general(qv, nb[...], (((1,), (1,)), ((), ())), preferred_element_type=F32)
    prod = (qf[0] * tb[0] + qf[1] * tb[1]) + (qf[2] * tb[2] + qf[3] * tb[3])
    p = jnp.sum(prod, axis=1, keepdims=True)
    top = jnp.maximum(jnp.max(s, axis=1, keepdims=True), p)
    p_exp = jnp.exp(p - top)
    s_exp = jnp.exp(s - top)
    total = p_exp + jnp.sum(s_exp, axis=1, keepdims=True)
    meta_v = meta[...]
    w = meta_v[:, 96:97].astype(F32)
    losses = w * ((top + jnp.log(total)) - p)
    loss_out[...] += jnp.broadcast_to(jnp.sum(losses, keepdims=True), loss_out.shape)
    dp = w * (p_exp / total - 1.0)
    ds = ((w / total) * s_exp).astype(BF16)
    dp_wide = jnp.broadcast_to(dp, (BLOCK, LANES))
    dp_out[0] = jnp.transpose(dp_wide)[0:1, :]
    gq = split_cols(jnp.dot(ds, nb[...], preferred_element_type=F32))
    gq = [dp_wide * tb[c] + gq[c] for c in range(4)]
    gneg_out[...] += lax.dot_general(ds, qv, (((0,), (0,)), ((), ())), preferred_element_type=F32)
    rr = split_cols(jnp.dot(meta_v, rel3[...], preferred_element_type=F32))
    gh = [gq[c] * rr[c] + gq[c + 2] * rr[c + 2] for c in (0, 1)]
    gh += [gq[c + 2] * rr[c] - gq[c] * rr[c + 2] for c in (0, 1)]
    gh_out[...] = flat_of(gh)
    e = chunks_of(eh[...])
    gr = [gq[c] * e[c] + gq[c + 2] * e[c + 2] for c in (0, 1)]
    gr += [gq[c + 2] * e[c] - gq[c] * e[c + 2] for c in (0, 1)]
    grel = jnp.zeros((LANES, 4 * LANES), F32)
    for piece in split3(jnp.concatenate(gr, axis=1)):
        grel += lax.dot_general(meta_v, piece, (((0,), (0,)), ((), ())), preferred_element_type=F32)
    grel_out[...] += grel[: grel_out.shape[0], :]


def update_kernel(h_ids, t_ids, n_ids, gh, qb, dp, gneg, ent, state, ent_out, state_out, bf_out, gt_buf, *accs, steps, rate):
    step = pl.program_id(0)
    h_accs, t_accs = accs[:ACCS], accs[ACCS:]

    @pl.when(step == 0)
    def _():
        def clear(g, carry):
            for acc in accs:
                acc[pl.ds(pl.multiple_of(g * 256, 256), 256), :] = jnp.zeros((256, LANES), F32)
            return carry

        lax.fori_loop(0, accs[0].shape[0] // 256, clear, 0)

    @pl.when(step < steps)
    def _():
        dp_wide = jnp.transpose(jnp.broadcast_to(dp[0], (LANES, BLOCK)))
        gt_buf[...] = flat_of([c * dp_wide for c in split_cols(qb[...].astype(F32))])

        def some(g, carry):
            base = g * (UNROLL // 2)
            for u in range(UNROLL // 2):
                src = row_at(base * 4 + (u // 8) * 32 + u % 8)
                k = step * BLOCK + base + u
                for ids, rows, group in ((h_ids, gh, h_accs), (t_ids, gt_buf, t_accs)):
                    acc = group[u % ACCS]
                    dst = row_at(ids[k])
                    acc[dst, :] = acc[dst, :] + rows[src, :]
            return carry

        lax.fori_loop(0, BLOCK // (UNROLL // 2), some, 0)

    @pl.when(step >= steps)
    def _():
        @pl.when(step == steps)
        def _():
            def some(g, carry):
                base = g * UNROLL
                for u in range(UNROLL):
                    acc = accs[u % len(accs)]
                    dst = row_at(n_ids[base + u])
                    acc[dst, :] = acc[dst, :] + gneg[row_at(base * 4 + (u // 8) * 32 + u % 8), :]
                return carry

            lax.fori_loop(0, n_ids.shape[0] // UNROLL, some, 0)

        rows = ent.shape[0]
        first = pl.multiple_of((step - steps) * rows, rows)
        grad = accs[0][pl.ds(first, rows), :]
        for acc in accs[1:]:
            grad = grad + acc[pl.ds(first, rows), :]
        g = chunks_of(grad)
        sq = (g[0] * g[0] + g[1] * g[1]) + (g[2] * g[2] + g[3] * g[3])
        new_state = state[...] + jnp.sum(sq, axis=1, keepdims=True) * (1.0 / (4 * LANES))
        state_out[...] = new_state
        scale = rate / jnp.sqrt(new_state + EPSILON)
        e = chunks_of(ent[...])
        e = flat_of([e[c] - scale * g[c] for c in range(4)])
        ent_out[...] = e
        bf_out[...] = e.astype(BF16)


SMEM = pl.BlockSpec(memory_space=pltpu.SMEM)
VMEM = pl.BlockSpec(memory_space=pltpu.VMEM)


def params(limit):
    return pltpu.CompilerParams(vmem_limit_bytes=limit * MIB, dimension_semantics=("arbitrary",))


def cost(micros):
    return pl.CostEstimate(flops=0, bytes_accessed=int(micros * 3e6), transcendentals=0)


def blocks(shape):
    return pl.BlockSpec(shape, lambda i: (i,) + (0,) * (len(shape) - 1))


def whole(shape):
    return pl.BlockSpec(shape, lambda i: (0,) * len(shape))


def shape_of(shape, dtype=F32):
    return jax.ShapeDtypeStruct(shape, dtype)


def run_heads(h_ids, table, meta, rel3):
    edges = h_ids.shape[0]
    return pl.pallas_call(
        head_kernel,
        grid=(edges // BLOCK,),
        out_shape=[shape_of((edges * 4, LANES)), shape_of((edges, 4 * LANES), BF16)],
        in_specs=[SMEM, VMEM, blocks((BLOCK, LANES)), VMEM],
        out_specs=[blocks((BLOCK * 4, LANES)), blocks((BLOCK, 4 * LANES))],
        compiler_params=params(32),
        cost_estimate=cost(12),
        name="heads",
    )(h_ids, table, meta, rel3)


def run_bucket(t_ids, n_ids, tail, qb, eh, meta, rel3):
    edges, negs = t_ids.shape[0], n_ids.shape[0]
    width = 4 * LANES
    return pl.pallas_call(
        bucket_kernel,
        grid=(edges // BLOCK,),
        out_shape=[
            shape_of((edges * 4, LANES)),
            shape_of((negs, width)),
            shape_of((edges // BLOCK, 1, BLOCK)),
            shape_of((24, width)),
            shape_of((8, LANES)),
        ],
        in_specs=[SMEM, SMEM, VMEM, blocks((BLOCK, width)), blocks((BLOCK * 4, LANES)), blocks((BLOCK, LANES)), VMEM],
        out_specs=[
            blocks((BLOCK * 4, LANES)),
            whole((negs, width)),
            blocks((1, 1, BLOCK)),
            whole((24, width)),
            whole((8, LANES)),
        ],
        scratch_shapes=[pltpu.VMEM(tail.shape, F32), pltpu.VMEM((negs, width), BF16), pltpu.VMEM((BLOCK * 4, LANES), F32)],
        compiler_params=params(48),
        cost_estimate=cost(40),
        name="bucket",
    )(t_ids, n_ids, tail, qb, eh, meta, rel3)


def run_update(h_ids, t_ids, n_ids, gh, qb, dp, gneg, ent, state, rate):
    edges = h_ids.shape[0]
    steps = edges // BLOCK
    flat_rows = ent.shape[0]
    out_steps = 16
    out_rows = flat_rows // out_steps
    early = lambda i: jnp.minimum(i, steps - 1)
    late = lambda i: jnp.maximum(i - steps, 0)
    late_block = lambda shape: pl.BlockSpec(shape, lambda i: (late(i), 0))
    return pl.pallas_call(
        functools.partial(update_kernel, steps=steps, rate=rate),
        grid=(steps + out_steps,),
        out_shape=[shape_of(ent.shape), shape_of(state.shape), shape_of(ent.shape, BF16)],
        in_specs=[
            SMEM,
            SMEM,
            SMEM,
            pl.BlockSpec((BLOCK * 4, LANES), lambda i: (early(i), 0)),
            pl.BlockSpec((BLOCK, 4 * LANES), lambda i: (early(i), 0)),
            pl.BlockSpec((1, 1, BLOCK), lambda i: (early(i), 0, 0)),
            VMEM,
            late_block((out_rows, LANES)),
            late_block((out_rows // 4, 1)),
        ],
        out_specs=[late_block((out_rows, LANES)), late_block((out_rows // 4, 1)), late_block((out_rows, LANES))],
        scratch_shapes=[pltpu.VMEM((BLOCK * 4, LANES), F32)] + [pltpu.VMEM((flat_rows, LANES), F32)] * (2 * ACCS),
        compiler_params=params(58),
        cost_estimate=cost(30),
        name="update",
    )(h_ids, t_ids, n_ids, gh, qb, dp, gneg, ent, state)


def rel_pieces(rel):
    hi = lax.reduce_precision(rel, 8, 7)
    mid = lax.reduce_precision(rel - hi, 8, 7)
    pieces = [jnp.pad(piece, ((0, 32 - rel.shape[0]), (0, 0))).astype(BF16) for piece in (hi, mid, (rel - hi) - mid)]
    return jnp.concatenate(pieces + [jnp.zeros((32, rel.shape[1]), BF16)], axis=0)


def solution(mesh):
    groups = mesh.shape['ent']
    row_spec = P(('sweep', 'ent'), None)
    edge_spec = P(('sweep', 'ent'), None, 'data')

    def device_fn(ent_table, ent_state, rel_table, head_idx, tail_idx, rel_idx, edge_mask, neg_idx):
        emb_width = ent_table.shape[1]
        rel_rows = rel_table.shape[0]
        rate = LR_SCALE * emb_width ** -0.25
        stacked = jnp.stack([head_idx[0], tail_idx[0], rel_idx[0], edge_mask[0]])
        both = lax.all_gather(stacked, 'data')
        both = both.transpose(1, 2, 0, 3).reshape(4, groups, -1)
        bucket_edges = both.shape[2]
        h_flat, t_flat = flat_row(both[0]), flat_row(both[1])
        n_flat = flat_row(neg_idx[0])
        rels, mask = both[2], both[3]
        lane = lax.broadcasted_iota(jnp.int32, (1, 1, LANES), 2)
        hit = ((lane & 31) == rels[:, :, None]) & (lane < 96)
        meta = jnp.where(lane == 96, mask[:, :, None], hit.astype(jnp.int32)).astype(BF16)

        def shift(value, step, back):
            sign = 1 if back else -1
            return lax.ppermute(value, 'ent', [(i, (i + sign * step) % groups) for i in range(groups)])

        in_tails = [t_flat[0]] + [shift(t_flat[s], s, True) for s in range(1, groups)]
        in_negs = [n_flat[0]] + [shift(n_flat[s], s, True) for s in range(1, groups)]

        ent = to_flat(ent_table)
        state = ent_state[:, None]
        ent_bf = ent.astype(BF16)
        rel, rel_state = rel_table, jnp.zeros((rel_rows,), F32)
        losses = []
        for s in range(groups):
            tail = ent_bf if s == 0 else shift(ent_bf, s, False)
            rel3 = rel_pieces(rel)
            eh, qb = run_heads(h_flat[s], ent, meta[s], rel3)
            qb_in = qb if s == 0 else shift(qb, s, True)
            gh, gneg, dp, grel, loss = run_bucket(t_flat[s], n_flat[s], tail, qb, eh, meta[s], rel3)
            losses.append(loss[0, 0] / bucket_edges)
            gneg = to_flat(gneg)
            gneg_in = gneg if s == 0 else shift(gneg, s, True)
            dp_in = dp if s == 0 else shift(dp, s, True)
            grel = lax.psum(grel[:rel_rows], 'ent')
            ent, state, ent_bf = run_update(h_flat[s], in_tails[s], in_negs[s], gh, qb_in, dp_in, gneg_in, ent, state, rate)
            rel_state = rel_state + jnp.mean(grel * grel, axis=-1)
            rel = rel - rate * (grel / jnp.sqrt(rel_state + EPSILON)[:, None])
        return from_flat(ent, emb_width // LANES), state[:, 0], rel, jnp.stack(losses)[None, :]

    return jax.shard_map(device_fn, mesh=mesh, in_specs=(row_spec, P(('sweep', 'ent')), P('sweep', None), edge_spec, edge_spec, edge_spec, edge_spec, P(('sweep', 'ent'), None, None)), out_specs=(row_spec, P(('sweep', 'ent')), P('sweep', None), row_spec), check_vma=False)
```

```python
import functools

import jax
import jax.numpy as jnp
from jax import lax
from jax.experimental import pallas as pl
from jax.experimental.pallas import tpu as pltpu
from jax.sharding import PartitionSpec as P

LR_SCALE = 0.2
EPSILON = 1e-8
LANES = 128
BLOCK = 512
UNROLL = 32
ACCS = 2
MIB = 2 ** 20
F32 = jnp.float32
BF16 = jnp.bfloat16


def to_flat(table):
    rows, width = table.shape
    parts = width // LANES
    return table.reshape(rows // 8, 8, parts, LANES).transpose(0, 2, 1, 3).reshape(rows * parts, LANES)


def from_flat(flat, parts):
    rows = flat.shape[0] // parts
    return flat.reshape(rows // 8, parts, 8, LANES).transpose(0, 2, 1, 3).reshape(rows, parts * LANES)


def flat_row(ids):
    return (ids >> 3) * 32 + (ids & 7)


def chunks_of(flat):
    groups = flat.shape[0] // 32
    cube = flat.reshape(groups, 32, LANES)
    return [cube[:, 8 * c : 8 * c + 8, :].reshape(groups * 8, LANES) for c in range(4)]


def flat_of(chunks):
    groups = chunks[0].shape[0] // 8
    cube = jnp.concatenate([c.reshape(groups, 8, LANES) for c in chunks], axis=1)
    return cube.reshape(groups * 32, LANES)


def split_cols(mat):
    return [mat[:, LANES * c : LANES * (c + 1)] for c in range(4)]


def split3(mat):
    hi = mat.astype(BF16)
    rest = mat - hi.astype(F32)
    mid = rest.astype(BF16)
    low = (rest - mid.astype(F32)).astype(BF16)
    return hi, mid, low


def row_at(start):
    return pl.ds(start, 4, stride=8)


def gather_rows(ids, first, count, table, out):
    def some(g, carry):
        base = g * UNROLL
        for u in range(UNROLL):
            out[row_at(base * 4 + (u // 8) * 32 + u % 8), :] = table[row_at(ids[first + base + u]), :]
        return carry

    lax.fori_loop(0, count // UNROLL, some, 0)


def head_kernel(ids, table, meta, rel3, eh_out, qb_out):
    step = pl.program_id(0)
    gather_rows(ids, step * BLOCK, BLOCK, table, eh_out)
    rr = split_cols(jnp.dot(meta[...], rel3[...], preferred_element_type=F32))
    eh = chunks_of(eh_out[...])
    q = [eh[c] * rr[c] - eh[c + 2] * rr[c + 2] for c in (0, 1)]
    q += [eh[c] * rr[c + 2] + eh[c + 2] * rr[c] for c in (0, 1)]
    qb_out[...] = jnp.concatenate(q, axis=1).astype(BF16)


def bucket_kernel(t_ids, n_ids, half, qb, eh, meta, rel3, *rest, plan):
    pieces, rest = rest[: sum(plan)], rest[sum(plan) :]
    gh_out, gneg_out, dp_out, grel_out, loss_out, table, nb, rows_buf = rest
    step = pl.program_id(0)

    @pl.when(step == 0)
    def _():
        at = 0
        for k, terms in enumerate(plan):
            rows = table.shape[0] // len(plan)
            first = k * rows
            if len(plan) > 1:
                own = half[0] if k < len(plan) // 2 else 1 - half[0]
                first = own * (table.shape[0] // 2) + (k % (len(plan) // 2)) * rows
            part = pieces[at : at + terms]
            at += terms

            def widen(g, carry):
                here = pl.ds(pl.multiple_of(g * 512, 512), 512)
                there = pl.ds(pl.multiple_of(first + g * 512, 512), 512)
                table[there, :] = sum((p[here, :].astype(F32) for p in part[1:]), part[0][here, :].astype(F32))
                return carry

            lax.fori_loop(0, rows // 512, widen, 0)
        negs = nb.shape[0]
        for first in range(0, negs, BLOCK):
            gather_rows(n_ids, first, BLOCK, table, rows_buf)
            nb[first : first + BLOCK, :] = jnp.concatenate(chunks_of(rows_buf[...]), axis=1).astype(BF16)
        gneg_out[...] = jnp.zeros_like(gneg_out)
        grel_out[...] = jnp.zeros_like(grel_out)
        loss_out[...] = jnp.zeros_like(loss_out)

    gather_rows(t_ids, step * BLOCK, BLOCK, table, rows_buf)
    tb = chunks_of(rows_buf[...])
    qv = qb[...]
    qf = split_cols(qv.astype(F32))
    s = lax.dot_general(qv, nb[...], (((1,), (1,)), ((), ())), preferred_element_type=F32)
    prod = (qf[0] * tb[0] + qf[1] * tb[1]) + (qf[2] * tb[2] + qf[3] * tb[3])
    p = jnp.sum(prod, axis=1, keepdims=True)
    top = jnp.maximum(jnp.max(s, axis=1, keepdims=True), p)
    p_exp = jnp.exp(p - top)
    s_exp = jnp.exp(s - top)
    total = p_exp + jnp.sum(s_exp, axis=1, keepdims=True)
    meta_v = meta[...]
    w = meta_v[:, 96:97].astype(F32)
    losses = w * ((top + jnp.log(total)) - p)
    loss_out[...] += jnp.broadcast_to(jnp.sum(losses, keepdims=True), loss_out.shape)
    dp = w * (p_exp / total - 1.0)
    ds = ((w / total) * s_exp).astype(BF16)
    dp_wide = jnp.broadcast_to(dp, (BLOCK, LANES))
    dp_out[0] = jnp.transpose(dp_wide)[0:1, :]
    gq = split_cols(jnp.dot(ds, nb[...], preferred_element_type=F32))
    gq = [dp_wide * tb[c] + gq[c] for c in range(4)]
    gneg_out[...] += lax.dot_general(ds, qv, (((0,), (0,)), ((), ())), preferred_element_type=F32)
    rr = split_cols(jnp.dot(meta_v, rel3[...], preferred_element_type=F32))
    gh = [gq[c] * rr[c] + gq[c + 2] * rr[c + 2] for c in (0, 1)]
    gh += [gq[c + 2] * rr[c] - gq[c] * rr[c + 2] for c in (0, 1)]
    gh_out[...] = flat_of(gh)
    e = chunks_of(eh[...])
    gr = [gq[c] * e[c] + gq[c + 2] * e[c + 2] for c in (0, 1)]
    gr += [gq[c + 2] * e[c] - gq[c] * e[c + 2] for c in (0, 1)]
    grel = jnp.zeros((LANES, 4 * LANES), F32)
    for piece in split3(jnp.concatenate(gr, axis=1)):
        grel += lax.dot_general(meta_v, piece, (((0,), (0,)), ((), ())), preferred_element_type=F32)
    grel_out[...] += grel[: grel_out.shape[0], :]


def scatter_kernel(h_ids, t_ids, half, gh, dp, *rest, steps, pieces):
    qbs, acc_out, gt_buf, accs = rest[:pieces], rest[pieces], rest[pieces + 1], rest[pieces + 2 :]
    step = pl.program_id(0)
    h_accs, t_accs = accs[:ACCS], accs[ACCS:]

    @pl.when(step == 0)
    def _():
        def clear(g, carry):
            for acc in accs:
                acc[pl.ds(pl.multiple_of(g * 256, 256), 256), :] = jnp.zeros((256, LANES), F32)
            return carry

        lax.fori_loop(0, accs[0].shape[0] // 256, clear, 0)

    @pl.when(step < steps)
    def _():
        dp_wide = jnp.transpose(jnp.broadcast_to(dp[0], (LANES, BLOCK)))
        qv = qbs[0][...]
        if pieces > 1:
            qv = jnp.where(step // (steps // pieces) == half[0], qv, qbs[1][...])
        gt_buf[...] = flat_of([c * dp_wide for c in split_cols(qv.astype(F32))])

        def some(g, carry):
            base = g * (UNROLL // 2)
            for u in range(UNROLL // 2):
                src = row_at(base * 4 + (u // 8) * 32 + u % 8)
                k = step * BLOCK + base + u
                for ids, rows, group in ((h_ids, gh, h_accs), (t_ids, gt_buf, t_accs)):
                    acc = group[u % ACCS]
                    dst = row_at(ids[k])
                    acc[dst, :] = acc[dst, :] + rows[src, :]
            return carry

        lax.fori_loop(0, BLOCK // (UNROLL // 2), some, 0)

    @pl.when(step >= steps)
    def _():
        rows = acc_out.shape[0]
        first = pl.multiple_of((step - steps) * rows, rows)
        grad = accs[0][pl.ds(first, rows), :]
        for acc in accs[1:]:
            grad = grad + acc[pl.ds(first, rows), :]
        acc_out[...] = grad


def update_kernel(n_ids, half, acc_in, ent, state, *rest, plan, rate):
    pieces, rest = rest[: sum(plan)], rest[sum(plan) :]
    ent_out, state_out, bf_out, acc = rest
    step = pl.program_id(0)

    @pl.when(step == 0)
    def _():
        def fetch(g, carry):
            here = pl.ds(pl.multiple_of(g * 512, 512), 512)
            acc[here, :] = acc_in[here, :]
            return carry

        lax.fori_loop(0, acc.shape[0] // 512, fetch, 0)
        at = 0
        count = n_ids.shape[0] // len(plan)
        for k, terms in enumerate(plan):
            part = pieces[at : at + terms]
            at += terms
            first = k * count
            if len(plan) > 1:
                first = (half[0] if k == 0 else 1 - half[0]) * count

            def some(g, carry):
                base = g * UNROLL
                for u in range(UNROLL):
                    dst = row_at(n_ids[first + base + u])
                    src = row_at(base * 4 + (u // 8) * 32 + u % 8)
                    acc[dst, :] = acc[dst, :] + sum((p[src, :] for p in part[1:]), part[0][src, :])
                return carry

            lax.fori_loop(0, count // UNROLL, some, 0)

    rows = ent.shape[0]
    g = chunks_of(acc[pl.ds(pl.multiple_of(step * rows, rows), rows), :])
    sq = (g[0] * g[0] + g[1] * g[1]) + (g[2] * g[2] + g[3] * g[3])
    new_state = state[...] + jnp.sum(sq, axis=1, keepdims=True) * (1.0 / (4 * LANES))
    state_out[...] = new_state
    scale = rate / jnp.sqrt(new_state + EPSILON)
    e = chunks_of(ent[...])
    e = flat_of([e[c] - scale * g[c] for c in range(4)])
    ent_out[...] = e
    bf_out[...] = e.astype(BF16)


SMEM = pl.BlockSpec(memory_space=pltpu.SMEM)
VMEM = pl.BlockSpec(memory_space=pltpu.VMEM)


def params(limit):
    return pltpu.CompilerParams(vmem_limit_bytes=limit * MIB, dimension_semantics=("arbitrary",))


def cost(micros):
    return pl.CostEstimate(flops=0, bytes_accessed=int(micros * 3e6), transcendentals=0)


def blocks(shape):
    return pl.BlockSpec(shape, lambda i: (i,) + (0,) * (len(shape) - 1))


def whole(shape):
    return pl.BlockSpec(shape, lambda i: (0,) * len(shape))


def shape_of(shape, dtype=F32):
    return jax.ShapeDtypeStruct(shape, dtype)


def run_heads(h_ids, table, meta, rel3):
    edges = h_ids.shape[0]
    return pl.pallas_call(
        head_kernel,
        grid=(edges // BLOCK,),
        out_shape=[shape_of((edges * 4, LANES)), shape_of((edges, 4 * LANES), BF16)],
        in_specs=[SMEM, VMEM, blocks((BLOCK, LANES)), VMEM],
        out_specs=[blocks((BLOCK * 4, LANES)), blocks((BLOCK, 4 * LANES))],
        compiler_params=params(32),
        cost_estimate=cost(12),
        name="heads",
    )(h_ids, table, meta, rel3)


def run_bucket(t_ids, n_ids, half, tail, qb, eh, meta, rel3):
    edges, negs = t_ids.shape[0], n_ids.shape[0]
    plan = tuple(len(piece) for piece in tail)
    flat = [array for piece in tail for array in piece]
    flat_rows = sum(piece[0].shape[0] for piece in tail)
    width = 4 * LANES
    return pl.pallas_call(
        functools.partial(bucket_kernel, plan=plan),
        grid=(edges // BLOCK,),
        out_shape=[
            shape_of((edges * 4, LANES)),
            shape_of((negs, width)),
            shape_of((edges // BLOCK, 1, BLOCK)),
            shape_of((24, width)),
            shape_of((8, LANES)),
        ],
        in_specs=[SMEM, SMEM, SMEM, blocks((BLOCK, width)), blocks((BLOCK * 4, LANES)), blocks((BLOCK, LANES)), VMEM] + [VMEM] * len(flat),
        out_specs=[
            blocks((BLOCK * 4, LANES)),
            whole((negs, width)),
            blocks((1, 1, BLOCK)),
            whole((24, width)),
            whole((8, LANES)),
        ],
        scratch_shapes=[pltpu.VMEM((flat_rows, LANES), F32), pltpu.VMEM((negs, width), BF16), pltpu.VMEM((BLOCK * 4, LANES), F32)],
        compiler_params=params(48),
        cost_estimate=cost(40),
        name="bucket",
    )(t_ids, n_ids, half, qb, eh, meta, rel3, *flat)


def run_scatter(h_ids, t_ids, half, gh, dp, qbs, flat_rows):
    edges = h_ids.shape[0]
    steps = edges // BLOCK
    out_steps = 8
    out_rows = flat_rows // out_steps
    early = lambda i: jnp.minimum(i, steps - 1)
    late = lambda i: jnp.maximum(i - steps, 0)
    return pl.pallas_call(
        functools.partial(scatter_kernel, steps=steps, pieces=len(qbs)),
        grid=(steps + out_steps,),
        out_shape=shape_of((flat_rows, LANES)),
        in_specs=[
            SMEM,
            SMEM,
            SMEM,
            pl.BlockSpec((BLOCK * 4, LANES), lambda i: (early(i), 0)),
            pl.BlockSpec((1, 1, BLOCK), lambda i: (early(i), 0, 0)),
        ]
        + [pl.BlockSpec((BLOCK, 4 * LANES), lambda i: (early(i) % (steps // len(qbs)), 0))] * len(qbs),
        out_specs=pl.BlockSpec((out_rows, LANES), lambda i: (late(i), 0)),
        scratch_shapes=[pltpu.VMEM((BLOCK * 4, LANES), F32)] + [pltpu.VMEM((flat_rows, LANES), F32)] * (2 * ACCS),
        compiler_params=params(48),
        cost_estimate=cost(25),
        name="scatter",
    )(h_ids, t_ids, half, gh, dp, *qbs)


def run_update(n_ids, half, acc, ent, state, gneg, rate):
    out_steps = 16
    out_rows = ent.shape[0] // out_steps
    plan = tuple(len(piece) for piece in gneg)
    flat = [array for piece in gneg for array in piece]
    return pl.pallas_call(
        functools.partial(update_kernel, plan=plan, rate=rate),
        grid=(out_steps,),
        out_shape=[shape_of(ent.shape), shape_of(state.shape), shape_of(ent.shape, BF16)],
        in_specs=[SMEM, SMEM, VMEM, blocks((out_rows, LANES)), blocks((out_rows // 4, 1))] + [VMEM] * len(flat),
        out_specs=[blocks((out_rows, LANES)), blocks((out_rows // 4, 1)), blocks((out_rows, LANES))],
        scratch_shapes=[pltpu.VMEM(ent.shape, F32)],
        compiler_params=params(40),
        cost_estimate=cost(12),
        name="update",
    )(n_ids, half, acc, ent, state, *flat)


def rel_pieces(rel):
    hi = lax.reduce_precision(rel, 8, 7)
    mid = lax.reduce_precision(rel - hi, 8, 7)
    pieces = [jnp.pad(piece, ((0, 32 - rel.shape[0]), (0, 0))).astype(BF16) for piece in (hi, mid, (rel - hi) - mid)]
    return jnp.concatenate(pieces + [jnp.zeros((32, rel.shape[1]), BF16)], axis=0)


def solution(mesh):
    groups = mesh.shape['ent']
    row_spec = P(('sweep', 'ent'), None)
    edge_spec = P(('sweep', 'ent'), None, 'data')

    def device_fn(ent_table, ent_state, rel_table, head_idx, tail_idx, rel_idx, edge_mask, neg_idx):
        emb_width = ent_table.shape[1]
        rel_rows = rel_table.shape[0]
        rate = LR_SCALE * emb_width ** -0.25
        stacked = jnp.stack([head_idx[0], tail_idx[0], rel_idx[0], edge_mask[0]])
        both = lax.all_gather(stacked, 'data')
        both = both.transpose(1, 2, 0, 3).reshape(4, groups, -1)
        bucket_edges = both.shape[2]
        h_flat, t_flat = flat_row(both[0]), flat_row(both[1])
        n_flat = flat_row(neg_idx[0])
        rels, mask = both[2], both[3]
        lane = lax.broadcasted_iota(jnp.int32, (1, 1, LANES), 2)
        hit = ((lane & 31) == rels[:, :, None]) & (lane < 96)
        meta = jnp.where(lane == 96, mask[:, :, None], hit.astype(jnp.int32)).astype(BF16)

        my_half = lax.axis_index('data')
        half = my_half.astype(jnp.int32)[None]

        def pairs_of(step, back):
            sign = 1 if back else -1
            return [(i, (i + sign * step) % groups) for i in range(groups)]

        def shift(value, step, back):
            return lax.ppermute(value, 'ent', pairs_of(step, back))

        def relayed(halves, step, back, parts):
            pairs = pairs_of(step, back)
            far = [(a, b) for a, b in pairs if a // 2 != b // 2]
            near = [(a, b) for a, b in pairs if a // 2 == b // 2]
            rows = halves.shape[1] // parts
            own = lax.dynamic_index_in_dim(halves, my_half, 0, keepdims=False)
            first = [shift(own[k * rows : (k + 1) * rows], step, back) for k in range(parts)]
            relay = [((1 - y) * groups + b, y * groups + b) for y in range(2) for _, b in far]
            second = [[lax.ppermute(piece, ('data', 'ent'), relay)] for piece in first]
            if near:
                direct = [(y * groups + a, y * groups + b) for y in range(2) for a, b in near]
                other = lax.dynamic_index_in_dim(halves, 1 - my_half, 0, keepdims=False)
                for k in range(parts):
                    second[k].append(lax.ppermute(other[k * rows : (k + 1) * rows], ('data', 'ent'), direct))
            return [[piece] for piece in first] + second

        def halved(value):
            return value.reshape(2, value.shape[0] // 2, *value.shape[1:])

        def group_sum(value):
            for mask in (1, 2):
                value = value + lax.ppermute(value, 'ent', [(i, i ^ mask) for i in range(groups)])
            return value

        in_tails = [t_flat[0]] + [shift(t_flat[s], s, True) for s in range(1, groups)]
        in_negs = [n_flat[0]] + [shift(n_flat[s], s, True) for s in range(1, groups)]

        ent = to_flat(ent_table)
        state = ent_state[:, None]
        ent_bf = ent.astype(BF16)
        rel, rel_state = rel_table, jnp.zeros((rel_rows,), F32)
        losses = []
        for s in range(groups):
            tail = [[ent_bf]] if s == 0 else relayed(halved(ent_bf), s, False, 4)
            rel3 = rel_pieces(rel)
            eh, qb = run_heads(h_flat[s], ent, meta[s], rel3)
            if s == 0:
                qbs = [qb]
            elif s == 2:
                qbs = [piece[0] for piece in relayed(halved(qb), s, True, 1)]
            else:
                qbs = [shift(qb, s, True)]
            gh, gneg, dp, grel, loss = run_bucket(t_flat[s], n_flat[s], half, tail, qb, eh, meta[s], rel3)
            losses.append(loss[0, 0] / bucket_edges)
            gneg = to_flat(gneg)
            gnegs = [[gneg]] if s == 0 else relayed(halved(gneg), s, True, 1)
            dp_in = dp if s == 0 else shift(dp, s, True)
            grel = group_sum(grel[:rel_rows])
            acc = run_scatter(h_flat[s], in_tails[s], half, gh, dp_in, qbs, ent.shape[0])
            ent, state, ent_bf = run_update(in_negs[s], half, acc, ent, state, gnegs, rate)
            rel_state = rel_state + jnp.mean(grel * grel, axis=-1)
            rel = rel - rate * (grel / jnp.sqrt(rel_state + EPSILON)[:, None])
        return from_flat(ent, emb_width // LANES), state[:, 0], rel, jnp.stack(losses)[None, :]

    return jax.shard_map(device_fn, mesh=mesh, in_specs=(row_spec, P(('sweep', 'ent')), P('sweep', None), edge_spec, edge_spec, edge_spec, edge_spec, P(('sweep', 'ent'), None, None)), out_specs=(row_spec, P(('sweep', 'ent')), P('sweep', None), row_spec), check_vma=False)
```

```python
import functools

import jax
import jax.numpy as jnp
from jax import lax
from jax.experimental import pallas as pl
from jax.experimental.pallas import tpu as pltpu
from jax.sharding import PartitionSpec as P

LR_SCALE = 0.2
EPSILON = 1e-8
LANES = 128
BLOCK = 512
UNROLL = 32
ACCS = 2
PARTS = 4
RATE = LR_SCALE * (4 * LANES) ** -0.25
MESH = pl.DeviceIdType.MESH
MIB = 2 ** 20
F32 = jnp.float32
BF16 = jnp.bfloat16


def to_flat(table):
    rows, width = table.shape
    parts = width // LANES
    return table.reshape(rows // 8, 8, parts, LANES).transpose(0, 2, 1, 3).reshape(rows * parts, LANES)


def from_flat(flat, parts):
    rows = flat.shape[0] // parts
    return flat.reshape(rows // 8, parts, 8, LANES).transpose(0, 2, 1, 3).reshape(rows, parts * LANES)


def flat_row(ids):
    return (ids >> 3) * 32 + (ids & 7)


def chunks_of(flat):
    groups = flat.shape[0] // 32
    cube = flat.reshape(groups, 32, LANES)
    return [cube[:, 8 * c : 8 * c + 8, :].reshape(groups * 8, LANES) for c in range(4)]


def flat_of(chunks):
    groups = chunks[0].shape[0] // 8
    cube = jnp.concatenate([c.reshape(groups, 8, LANES) for c in chunks], axis=1)
    return cube.reshape(groups * 32, LANES)


def split_cols(mat):
    return [mat[:, LANES * c : LANES * (c + 1)] for c in range(4)]


def split3(mat):
    hi = mat.astype(BF16)
    rest = mat - hi.astype(F32)
    mid = rest.astype(BF16)
    low = (rest - mid.astype(F32)).astype(BF16)
    return hi, mid, low


def row_at(start):
    return pl.ds(start, 4, stride=8)


def gather_rows(ids, first, count, table, out):
    def some(g, carry):
        base = g * UNROLL
        for u in range(UNROLL):
            out[row_at(base * 4 + (u // 8) * 32 + u % 8), :] = table[row_at(ids[first + base + u]), :]
        return carry

    lax.fori_loop(0, count // UNROLL, some, 0)


def round_kernel(*refs, shift, groups):
    remote = shift > 0
    h_ids, t_ids, n_ids, ent, meta, rel, rel_state, grel_in = refs[:8]
    refs = refs[8:]
    if remote:
        ent_bf, refs = refs[0], refs[1:]
    gh_out, gneg_out, dp_out, grel_out, loss_out, rel_out, rel_state_out = refs[:7]
    refs = refs[7:]
    qb_in, refs = refs[0], refs[1:]
    table, eh_buf, qb_buf, nb, rows_buf, rel3, gh_sem = refs[:7]
    refs = refs[7:]
    edges = qb_buf.shape[0]
    count = edges // BLOCK

    if remote:
        tail, grels, g_send, g_recv, t_send, t_relay, t_recv, q_send, q_relay, q_recv = refs
        me, my_half = lax.axis_index('ent'), lax.axis_index('data')
        other_half = 1 - my_half
        before, after = lax.rem(me + groups - shift, groups), lax.rem(me + shift, groups)
        far_before = (before // 2) != (me // 2)
        far_after = (after // 2) != (me // 2)

        barrier = pltpu.get_barrier_semaphore()
        for dy in range(2):
            for de in range(groups):
                if dy or de:
                    peer = {'data': lax.rem(my_half + dy, 2), 'ent': lax.rem(me + de, groups)}
                    pl.semaphore_signal(barrier, inc=1, device_id=peer, device_id_type=MESH)
        pl.semaphore_wait(barrier, 2 * groups - 1)

        def table_copy(c, source, sem, peer):
            rows = pl.ds(pl.multiple_of(c * (tail.shape[0] // (2 * PARTS)), 256), tail.shape[0] // (2 * PARTS))
            return pltpu.make_async_remote_copy(source.at[rows], tail.at[rows], sem, t_recv.at[c], device_id=peer, device_id_type=MESH)

        def query_copy(c, source, sem, peer):
            rows = pl.ds(pl.multiple_of(c * (edges // (2 * PARTS)), 128), edges // (2 * PARTS))
            return pltpu.make_async_remote_copy(source.at[rows], qb_in.at[rows], sem, q_recv.at[c], device_id=peer, device_id_type=MESH)

        def send(copy, source, sems, far, peer, go):
            @pl.when(far)
            def _():
                for k in range(PARTS):
                    go(copy(my_half * PARTS + k, source, sems.at[k], {'ent': peer}))

            @pl.when(jnp.logical_not(far))
            def _():
                for c in range(2 * PARTS):
                    go(copy(c, source, sems.at[c], {'ent': peer}))

        def start(copy):
            copy.start()

        def sent(copy):
            copy.wait_send()

        def rel_copy(de):
            return pltpu.make_async_remote_copy(grel_in, grels.at[me], g_send.at[de - 1], g_recv.at[de - 1], device_id={'ent': lax.rem(me + de, groups)}, device_id_type=MESH)

        for de in range(1, groups):
            rel_copy(de).start()
        send(table_copy, ent_bf, t_send, far_before, before, start)
        grels[me] = grel_in[...]
        for de in range(1, groups):
            rel_copy(de).wait()
        grel = (grels[0] + grels[1]) + (grels[2] + grels[3])
        state = rel_state[...] + jnp.mean(grel * grel, axis=1, keepdims=True)
        rel_now = rel[...] - RATE * (grel / jnp.sqrt(state + EPSILON))
        rel_state_out[...] = state
        rel_out[...] = rel_now
    else:
        rel_now = rel[...]
        rel_out[...] = rel_now
        rel_state_out[...] = rel_state[...]
    rel3[...] = jnp.concatenate(list(split3(rel_now)) + [jnp.zeros(rel.shape, BF16)], axis=0)

    def rel_of(blk):
        hits = meta[pl.ds(pl.multiple_of(blk * BLOCK, BLOCK), BLOCK), :]
        return hits, split_cols(jnp.dot(hits, rel3[...], preferred_element_type=F32))

    def flat_block(blk):
        return pl.ds(pl.multiple_of(blk * (BLOCK * 4), BLOCK * 4), BLOCK * 4)

    def heads(blk, carry):
        gather_rows(h_ids, blk * BLOCK, BLOCK, ent, rows_buf)
        rows = rows_buf[...]
        eh_buf[flat_block(blk), :] = rows
        _, rr = rel_of(blk)
        eh = chunks_of(rows)
        q = [eh[c] * rr[c] - eh[c + 2] * rr[c + 2] for c in (0, 1)]
        q += [eh[c] * rr[c + 2] + eh[c + 2] * rr[c] for c in (0, 1)]
        qb_buf[pl.ds(pl.multiple_of(blk * BLOCK, BLOCK), BLOCK), :] = jnp.concatenate(q, axis=1).astype(BF16)
        return carry

    lax.fori_loop(0, count, heads, 0)

    def widen(source, first, rows):
        def some(g, carry):
            here = pl.ds(pl.multiple_of(first + g * 512, 512), 512)
            table[here, :] = source[here, :].astype(BF16).astype(F32)
            return carry

        lax.fori_loop(0, rows // 512, some, 0)

    if remote:
        send(query_copy, qb_buf, q_send, far_after, after, start)
        rows = tail.shape[0] // (2 * PARTS)
        for k in range(PARTS):
            c = my_half * PARTS + k
            table_copy(c, tail, t_relay.at[k], {'data': other_half}).wait_recv()

            @pl.when(far_after)
            def _():
                table_copy(c, tail, t_relay.at[k], {'data': other_half}).start()

            widen(tail, c * rows, rows)
        for k in range(PARTS):
            c = other_half * PARTS + k
            table_copy(c, tail, t_relay.at[k], {'data': other_half}).wait_recv()
            widen(tail, c * rows, rows)
    else:
        widen(ent, 0, table.shape[0])

    for first in range(0, nb.shape[0], BLOCK):
        gather_rows(n_ids, first, BLOCK, table, rows_buf)
        nb[first : first + BLOCK, :] = jnp.concatenate(chunks_of(rows_buf[...]), axis=1).astype(BF16)
    gneg_out[...] = jnp.zeros_like(gneg_out)
    grel_out[...] = jnp.zeros_like(grel_out)
    loss_out[...] = jnp.zeros_like(loss_out)

    def gh_copy(blk):
        return pltpu.make_async_copy(eh_buf.at[flat_block(blk)], gh_out.at[flat_block(blk)], gh_sem.at[blk])

    def bucket(blk):
        gather_rows(t_ids, blk * BLOCK, BLOCK, table, rows_buf)
        tb = chunks_of(rows_buf[...])
        qv = qb_buf[pl.ds(pl.multiple_of(blk * BLOCK, BLOCK), BLOCK), :]
        qf = split_cols(qv.astype(F32))
        s = lax.dot_general(qv, nb[...], (((1,), (1,)), ((), ())), preferred_element_type=F32)
        prod = (qf[0] * tb[0] + qf[1] * tb[1]) + (qf[2] * tb[2] + qf[3] * tb[3])
        p = jnp.sum(prod, axis=1, keepdims=True)
        top = jnp.maximum(jnp.max(s, axis=1, keepdims=True), p)
        p_exp = jnp.exp(p - top)
        s_exp = jnp.exp(s - top)
        total = p_exp + jnp.sum(s_exp, axis=1, keepdims=True)
        hits, rr = rel_of(blk)
        w = hits[:, 96:97].astype(F32)
        losses = w * ((top + jnp.log(total)) - p)
        loss_out[...] += jnp.broadcast_to(jnp.sum(losses, keepdims=True), loss_out.shape)
        dp = w * (p_exp / total - 1.0)
        ds = ((w / total) * s_exp).astype(BF16)
        dp_wide = jnp.broadcast_to(dp, (BLOCK, LANES))
        dp_out[blk] = jnp.transpose(dp_wide)[0:1, :]
        gq = split_cols(jnp.dot(ds, nb[...], preferred_element_type=F32))
        gq = [dp_wide * tb[c] + gq[c] for c in range(4)]
        gneg_out[...] += lax.dot_general(ds, qv, (((0,), (0,)), ((), ())), preferred_element_type=F32)
        e = chunks_of(eh_buf[flat_block(blk), :])
        gr = [gq[c] * e[c] + gq[c + 2] * e[c + 2] for c in (0, 1)]
        gr += [gq[c + 2] * e[c] - gq[c] * e[c + 2] for c in (0, 1)]
        grel = jnp.zeros((LANES, 4 * LANES), F32)
        for piece in split3(jnp.concatenate(gr, axis=1)):
            grel += lax.dot_general(hits, piece, (((0,), (0,)), ((), ())), preferred_element_type=F32)
        grel_out[...] += grel[: grel_out.shape[0], :]
        gh = [gq[c] * rr[c] + gq[c + 2] * rr[c + 2] for c in (0, 1)]
        gh += [gq[c + 2] * rr[c] - gq[c] * rr[c + 2] for c in (0, 1)]
        eh_buf[flat_block(blk), :] = flat_of(gh)
        gh_copy(blk).start()

    def some(k, carry):
        def each(i, carry):
            bucket(k * (count // PARTS) + i)
            return carry

        lax.fori_loop(0, count // PARTS, each, 0)
        if remote:
            c = my_half * PARTS + k
            query_copy(c, qb_in, q_relay.at[k], {'data': other_half}).wait_recv()

            @pl.when(far_before)
            def _():
                query_copy(c, qb_in, q_relay.at[k], {'data': other_half}).start()

        return carry

    if not remote:
        pltpu.make_async_copy(qb_buf, qb_in, gh_sem.at[count]).start()
    lax.fori_loop(0, PARTS, some, 0)
    for blk in range(count):
        gh_copy(blk).wait()
    if not remote:
        pltpu.make_async_copy(qb_buf, qb_in, gh_sem.at[count]).wait()
    if remote:
        for k in range(PARTS):
            query_copy(other_half * PARTS + k, qb_in, q_relay.at[k], {'data': other_half}).wait_recv()
        send(table_copy, ent_bf, t_send, far_before, before, sent)
        send(query_copy, qb_buf, q_send, far_after, after, sent)

        @pl.when(far_after)
        def _():
            for k in range(PARTS):
                table_copy(my_half * PARTS + k, tail, t_relay.at[k], {'data': other_half}).wait_send()

        @pl.when(far_before)
        def _():
            for k in range(PARTS):
                query_copy(my_half * PARTS + k, qb_in, q_relay.at[k], {'data': other_half}).wait_send()


def scatter_kernel(h_ids, t_ids, half, gh, dp, *rest, steps, pieces):
    qbs, acc_out, gt_buf, accs = rest[:pieces], rest[pieces], rest[pieces + 1], rest[pieces + 2 :]
    step = pl.program_id(0)
    h_accs, t_accs = accs[:ACCS], accs[ACCS:]

    @pl.when(step == 0)
    def _():
        def clear(g, carry):
            for acc in accs:
                acc[pl.ds(pl.multiple_of(g * 256, 256), 256), :] = jnp.zeros((256, LANES), F32)
            return carry

        lax.fori_loop(0, accs[0].shape[0] // 256, clear, 0)

    @pl.when(step < steps)
    def _():
        dp_wide = jnp.transpose(jnp.broadcast_to(dp[0], (LANES, BLOCK)))
        qv = qbs[0][...]
        if pieces > 1:
            qv = jnp.where(step // (steps // pieces) == half[0], qv, qbs[1][...])
        gt_buf[...] = flat_of([c * dp_wide for c in split_cols(qv.astype(F32))])

        def some(g, carry):
            base = g * (UNROLL // 2)
            for u in range(UNROLL // 2):
                src = row_at(base * 4 + (u // 8) * 32 + u % 8)
                k = step * BLOCK + base + u
                for ids, rows, group in ((h_ids, gh, h_accs), (t_ids, gt_buf, t_accs)):
                    acc = group[u % ACCS]
                    dst = row_at(ids[k])
                    acc[dst, :] = acc[dst, :] + rows[src, :]
            return carry

        lax.fori_loop(0, BLOCK // (UNROLL // 2), some, 0)

    @pl.when(step >= steps)
    def _():
        rows = acc_out.shape[0]
        first = pl.multiple_of((step - steps) * rows, rows)
        grad = accs[0][pl.ds(first, rows), :]
        for acc in accs[1:]:
            grad = grad + acc[pl.ds(first, rows), :]
        acc_out[...] = grad


def update_kernel(n_ids, half, acc_in, ent, state, *rest, plan, rate):
    pieces, rest = rest[: sum(plan)], rest[sum(plan) :]
    ent_out, state_out, bf_out, acc = rest
    step = pl.program_id(0)

    @pl.when(step == 0)
    def _():
        def fetch(g, carry):
            here = pl.ds(pl.multiple_of(g * 512, 512), 512)
            acc[here, :] = acc_in[here, :]
            return carry

        lax.fori_loop(0, acc.shape[0] // 512, fetch, 0)
        at = 0
        count = n_ids.shape[0] // len(plan)
        for k, terms in enumerate(plan):
            part = pieces[at : at + terms]
            at += terms
            first = k * count
            if len(plan) > 1:
                first = (half[0] if k == 0 else 1 - half[0]) * count

            def some(g, carry):
                base = g * UNROLL
                for u in range(UNROLL):
                    dst = row_at(n_ids[first + base + u])
                    src = row_at(base * 4 + (u // 8) * 32 + u % 8)
                    acc[dst, :] = acc[dst, :] + sum((p[src, :] for p in part[1:]), part[0][src, :])
                return carry

            lax.fori_loop(0, count // UNROLL, some, 0)

    rows = ent.shape[0]
    g = chunks_of(acc[pl.ds(pl.multiple_of(step * rows, rows), rows), :])
    sq = (g[0] * g[0] + g[1] * g[1]) + (g[2] * g[2] + g[3] * g[3])
    new_state = state[...] + jnp.sum(sq, axis=1, keepdims=True) * (1.0 / (4 * LANES))
    state_out[...] = new_state
    scale = rate / jnp.sqrt(new_state + EPSILON)
    e = chunks_of(ent[...])
    e = flat_of([e[c] - scale * g[c] for c in range(4)])
    ent_out[...] = e
    bf_out[...] = e.astype(BF16)


ANY = pl.BlockSpec(memory_space=pl.ANY)
SMEM = pl.BlockSpec(memory_space=pltpu.SMEM)
VMEM = pl.BlockSpec(memory_space=pltpu.VMEM)


def params(limit):
    return pltpu.CompilerParams(vmem_limit_bytes=limit * MIB, dimension_semantics=("arbitrary",))


def cost(micros):
    return pl.CostEstimate(flops=0, bytes_accessed=int(micros * 3e6), transcendentals=0)


def blocks(shape):
    return pl.BlockSpec(shape, lambda i: (i,) + (0,) * (len(shape) - 1))


def whole(shape):
    return pl.BlockSpec(shape, lambda i: (0,) * len(shape))


def shape_of(shape, dtype=F32):
    return jax.ShapeDtypeStruct(shape, dtype)


def run_round(shift, groups, h_ids, t_ids, n_ids, ent, ent_bf, meta, rel, rel_state, grel):
    edges, negs, width = h_ids.shape[0], n_ids.shape[0], 4 * LANES
    count = edges // BLOCK
    remote = shift > 0
    dma = pltpu.SemaphoreType.DMA
    out_shape = [
        shape_of((edges * 4, LANES)),
        shape_of((negs, width)),
        shape_of((count, 1, BLOCK)),
        shape_of(rel.shape),
        shape_of((8, LANES)),
        shape_of(rel.shape),
        shape_of(rel_state.shape),
        shape_of((edges, width), BF16),
    ]
    out_specs = [ANY] + [VMEM] * 6 + [ANY]
    scratch = [
        pltpu.VMEM(ent.shape, F32),
        pltpu.VMEM((edges * 4, LANES), F32),
        pltpu.VMEM((edges, width), BF16),
        pltpu.VMEM((negs, width), BF16),
        pltpu.VMEM((BLOCK * 4, LANES), F32),
        pltpu.VMEM((LANES, width), BF16),
        dma((count + 1,)),
    ]
    args = [h_ids, t_ids, n_ids, ent, meta, rel, rel_state, grel]
    in_specs = [SMEM] * 3 + [VMEM] * 5
    if remote:
        args.append(ent_bf)
        in_specs.append(ANY)
        scratch += [pltpu.VMEM(ent.shape, BF16), pltpu.VMEM((groups,) + rel.shape, F32)]
        scratch += [dma((groups - 1,))] * 2 + [dma((2 * PARTS,)), dma((PARTS,)), dma((2 * PARTS,))] * 2
    return pl.pallas_call(
        functools.partial(round_kernel, shift=shift, groups=groups),
        out_shape=out_shape,
        in_specs=in_specs,
        out_specs=out_specs,
        scratch_shapes=scratch,
        compiler_params=pltpu.CompilerParams(
            vmem_limit_bytes=60 * MIB,
            collective_id=shift if remote else None,
            has_side_effects=remote,
        ),
        cost_estimate=cost(60),
        name="round",
    )(*args)


def run_scatter(h_ids, t_ids, half, gh, dp, qbs, flat_rows):
    edges = h_ids.shape[0]
    steps = edges // BLOCK
    out_steps = 8
    out_rows = flat_rows // out_steps
    early = lambda i: jnp.minimum(i, steps - 1)
    late = lambda i: jnp.maximum(i - steps, 0)
    return pl.pallas_call(
        functools.partial(scatter_kernel, steps=steps, pieces=len(qbs)),
        grid=(steps + out_steps,),
        out_shape=shape_of((flat_rows, LANES)),
        in_specs=[
            SMEM,
            SMEM,
            SMEM,
            pl.BlockSpec((BLOCK * 4, LANES), lambda i: (early(i), 0)),
            pl.BlockSpec((1, 1, BLOCK), lambda i: (early(i), 0, 0)),
        ]
        + [pl.BlockSpec((BLOCK, 4 * LANES), lambda i: (early(i) % (steps // len(qbs)), 0))] * len(qbs),
        out_specs=pl.BlockSpec((out_rows, LANES), lambda i: (late(i), 0)),
        scratch_shapes=[pltpu.VMEM((BLOCK * 4, LANES), F32)] + [pltpu.VMEM((flat_rows, LANES), F32)] * (2 * ACCS),
        compiler_params=params(48),
        cost_estimate=cost(25),
        name="scatter",
    )(h_ids, t_ids, half, gh, dp, *qbs)


def run_update(n_ids, half, acc, ent, state, gneg, rate):
    out_steps = 16
    out_rows = ent.shape[0] // out_steps
    plan = tuple(len(piece) for piece in gneg)
    flat = [array for piece in gneg for array in piece]
    return pl.pallas_call(
        functools.partial(update_kernel, plan=plan, rate=rate),
        grid=(out_steps,),
        out_shape=[shape_of(ent.shape), shape_of(state.shape), shape_of(ent.shape, BF16)],
        in_specs=[SMEM, SMEM, VMEM, blocks((out_rows, LANES)), blocks((out_rows // 4, 1))] + [VMEM] * len(flat),
        out_specs=[blocks((out_rows, LANES)), blocks((out_rows // 4, 1)), blocks((out_rows, LANES))],
        scratch_shapes=[pltpu.VMEM(ent.shape, F32)],
        compiler_params=params(40),
        cost_estimate=cost(12),
        name="update",
    )(n_ids, half, acc, ent, state, *flat)


def solution(mesh):
    groups = mesh.shape['ent']
    row_spec = P(('sweep', 'ent'), None)
    edge_spec = P(('sweep', 'ent'), None, 'data')

    def device_fn(ent_table, ent_state, rel_table, head_idx, tail_idx, rel_idx, edge_mask, neg_idx):
        emb_width = ent_table.shape[1]
        rel_rows = rel_table.shape[0]
        stacked = jnp.stack([head_idx[0], tail_idx[0], rel_idx[0], edge_mask[0]])
        both = lax.all_gather(stacked, 'data')
        both = both.transpose(1, 2, 0, 3).reshape(4, groups, -1)
        bucket_edges = both.shape[2]
        h_flat, t_flat = flat_row(both[0]), flat_row(both[1])
        n_flat = flat_row(neg_idx[0])
        rels, mask = both[2], both[3]
        lane = lax.broadcasted_iota(jnp.int32, (1, 1, LANES), 2)
        hit = ((lane & 31) == rels[:, :, None]) & (lane < 96)
        meta = jnp.where(lane == 96, mask[:, :, None], hit.astype(jnp.int32)).astype(BF16)

        my_half = lax.axis_index('data')
        half = my_half.astype(jnp.int32)[None]

        def pairs_of(step, back):
            sign = 1 if back else -1
            return [(i, (i + sign * step) % groups) for i in range(groups)]

        def shift(value, step, back):
            return lax.ppermute(value, 'ent', pairs_of(step, back))

        def group_sum(value):
            for mask in (1, 2):
                value = value + lax.ppermute(value, 'ent', [(i, i ^ mask) for i in range(groups)])
            return value

        in_tails = [t_flat[0]] + [shift(t_flat[s], s, True) for s in range(1, groups)]
        in_negs = [n_flat[0]] + [shift(n_flat[s], s, True) for s in range(1, groups)]

        ent = to_flat(ent_table)
        state = ent_state[:, None]
        ent_bf = None
        rel = jnp.pad(rel_table, ((0, 32 - rel_rows), (0, 0)))
        rel_state = jnp.zeros((32, 1), F32)
        grel = jnp.zeros_like(rel)
        losses = []
        for s in range(groups):
            gh, gneg, dp, grel, loss, rel, rel_state, *rest = run_round(
                s, groups, h_flat[s], t_flat[s], n_flat[s], ent, ent_bf, meta[s], rel, rel_state, grel
            )
            losses.append(loss[0, 0] / bucket_edges)
            gneg = to_flat(gneg)
            if s == 0:
                gneg_in, dp_in, qb_in = gneg, dp, rest[0]
            else:
                gneg_in, dp_in, qb_in = shift(gneg, s, True), shift(dp, s, True), rest[0]
            acc = run_scatter(h_flat[s], in_tails[s], half, gh, dp_in, [qb_in], ent.shape[0])
            ent, state, ent_bf = run_update(in_negs[s], half, acc, ent, state, [[gneg_in]], RATE)
        grel = group_sum(grel)
        rel_state = rel_state + jnp.mean(grel * grel, axis=1, keepdims=True)
        rel = (rel - RATE * (grel / jnp.sqrt(rel_state + EPSILON)))[:rel_rows]
        return from_flat(ent, emb_width // LANES), state[:, 0], rel, jnp.stack(losses)[None, :]

    return jax.shard_map(device_fn, mesh=mesh, in_specs=(row_spec, P(('sweep', 'ent')), P('sweep', None), edge_spec, edge_spec, edge_spec, edge_spec, P(('sweep', 'ent'), None, None)), out_specs=(row_spec, P(('sweep', 'ent')), P('sweep', None), row_spec), check_vma=False)
```

```python
import functools

import jax
import jax.numpy as jnp
from jax import lax
from jax.experimental import pallas as pl
from jax.experimental.pallas import tpu as pltpu
from jax.sharding import PartitionSpec as P

LR_SCALE = 0.2
EPSILON = 1e-8
LANES = 128
BLOCK = 512
UNROLL = 32
PARTS = 8
NEG_PARTS = 4
RATE = LR_SCALE * (4 * LANES) ** -0.25
MESH = pl.DeviceIdType.MESH
MIB = 2 ** 20
F32 = jnp.float32
BF16 = jnp.bfloat16


def to_flat(table):
    rows, width = table.shape
    parts = width // LANES
    return table.reshape(rows // 8, 8, parts, LANES).transpose(0, 2, 1, 3).reshape(rows * parts, LANES)


def from_flat(flat, parts):
    rows = flat.shape[0] // parts
    return flat.reshape(rows // 8, parts, 8, LANES).transpose(0, 2, 1, 3).reshape(rows, parts * LANES)


def flat_row(ids):
    return (ids >> 3) * 32 + (ids & 7)


def chunks_of(flat):
    groups = flat.shape[0] // 32
    cube = flat.reshape(groups, 32, LANES)
    return [cube[:, 8 * c : 8 * c + 8, :].reshape(groups * 8, LANES) for c in range(4)]


def flat_of(chunks):
    groups = chunks[0].shape[0] // 8
    cube = jnp.concatenate([c.reshape(groups, 8, LANES) for c in chunks], axis=1)
    return cube.reshape(groups * 32, LANES)


def split_cols(mat):
    return [mat[:, LANES * c : LANES * (c + 1)] for c in range(4)]


def split3(mat):
    hi = mat.astype(BF16)
    rest = mat - hi.astype(F32)
    mid = rest.astype(BF16)
    low = (rest - mid.astype(F32)).astype(BF16)
    return hi, mid, low


def row_at(start):
    return pl.ds(start, 4, stride=8)


def gather_rows(ids, first, count, table, out):
    def some(g, carry):
        base = g * UNROLL
        for u in range(UNROLL):
            out[row_at(base * 4 + (u // 8) * 32 + u % 8), :] = table[row_at(ids[first + base + u]), :]
        return carry

    lax.fori_loop(0, count // UNROLL, some, 0)


def adagrad(ent, state, grad):
    g = chunks_of(grad)
    sq = (g[0] * g[0] + g[1] * g[1]) + (g[2] * g[2] + g[3] * g[3])
    new_state = state + jnp.sum(sq, axis=1, keepdims=True) * (1.0 / (4 * LANES))
    scale = RATE / jnp.sqrt(new_state + EPSILON)
    e = chunks_of(ent)
    return flat_of([e[c] - scale * g[c] for c in range(4)]), new_state


def round_kernel(*refs, shift, groups):
    remote = shift > 0
    h_ids, t_ids, n_ids, ent, meta, rel, rel_state, grel_in = refs[:8]
    refs = refs[8:]
    if remote:
        acc, state, refs = refs[0], refs[1], refs[2:]
    gh_out, gneg_in, dp_in, grel_out, loss_out, rel_out, rel_state_out, qb_in = refs[:8]
    refs = refs[8:]
    dp_out = dp_in
    if remote:
        ent_out, state_out, refs = refs[0], refs[1], refs[2:]
    ent_v, table, eh_buf, qb_buf, nb, rows_buf, rel3, gneg_buf, gh_sem, ld_sem = refs[:10]
    refs = refs[10:]
    edges, negs = qb_buf.shape[0], nb.shape[0]
    count = edges // BLOCK
    part_rows = ent_v.shape[0] // (2 * PARTS)

    def part(c):
        return pl.ds(pl.multiple_of(c * part_rows, part_rows), part_rows)

    if remote:
        tail, tbf, grels, dp_out, ac_sem, out_sem, dp_send, dp_recv, g_send, g_recv = refs[:10]
        t_send, t_relay, t_recv, q_send, q_relay, q_recv, n_send, n_relay, n_recv = refs[10:]
        me, my_half = lax.axis_index('ent'), lax.axis_index('data')
        other_half = 1 - my_half
        before, after = lax.rem(me + groups - shift, groups), lax.rem(me + shift, groups)
        far_before = (before // 2) != (me // 2)
        far_after = (after // 2) != (me // 2)
        near_before, near_after = jnp.logical_not(far_before), jnp.logical_not(far_after)

        def loads(c):
            return (
                pltpu.make_async_copy(ent.at[part(c)], ent_v.at[part(c)], ld_sem.at[c]),
                pltpu.make_async_copy(acc.at[part(c)], table.at[part(c)], ac_sem.at[c]),
            )

        for side in (my_half, other_half):
            for k in range(PARTS):
                for copy in loads(side * PARTS + k):
                    copy.start()

        barrier = pltpu.get_barrier_semaphore()
        for dy in range(2):
            for de in range(groups):
                if dy or de:
                    peer = {'data': lax.rem(my_half + dy, 2), 'ent': lax.rem(me + de, groups)}
                    pl.semaphore_signal(barrier, inc=1, device_id=peer, device_id_type=MESH)
        pl.semaphore_wait(barrier, 2 * groups - 1)

        def rel_copy(de):
            return pltpu.make_async_remote_copy(grel_in, grels.at[me], g_send.at[de - 1], g_recv.at[de - 1], device_id={'ent': lax.rem(me + de, groups)}, device_id_type=MESH)

        for de in range(1, groups):
            rel_copy(de).start()
        grels[me] = grel_in[...]

        def piece_copy(source, target, rows, send_sem, recv_sem, c, peer):
            here = pl.ds(pl.multiple_of(c * rows, rows), rows)
            return pltpu.make_async_remote_copy(source.at[here], target.at[here], send_sem, recv_sem.at[c], device_id=peer, device_id_type=MESH)

        def table_copy(c, source, sem, peer):
            return piece_copy(source, tail, part_rows, sem, t_recv, c, peer)

        def query_copy(c, source, sem, peer):
            return piece_copy(source, qb_in, edges // (2 * PARTS), sem, q_recv, c, peer)

        def neg_copy(c, source, sem, peer):
            return piece_copy(source, gneg_in, negs // (2 * NEG_PARTS), sem, n_recv, c, peer)

        def send(copy, source, sems, far, peer, parts, go):
            @pl.when(far)
            def _():
                for k in range(parts):
                    go(copy(my_half * parts + k, source, sems.at[my_half * parts + k], {'ent': peer}))

            @pl.when(jnp.logical_not(far))
            def _():
                for c in range(2 * parts):
                    go(copy(c, source, sems.at[c], {'ent': peer}))

        def start(copy):
            copy.start()

        def sent(copy):
            copy.wait_send()

        def send_part(c):
            table_copy(c, tbf, t_send.at[c], {'ent': before}).start()

        def update(c):
            for copy in loads(c):
                copy.wait()
            rows = pl.ds(pl.multiple_of(c * (part_rows // 4), part_rows // 4), part_rows // 4)
            new_rows, new_state = adagrad(ent_v[part(c), :], state[rows, :], table[part(c), :])
            state_out[rows, :] = new_state
            ent_v[part(c), :] = new_rows
            tbf[part(c), :] = new_rows.astype(BF16)

        def own(k, carry):
            update(my_half * PARTS + k)

            @pl.when(k > 0)
            def _():
                send_part(my_half * PARTS + k - 1)

            return carry

        def others(k, carry):
            update(other_half * PARTS + k)

            @pl.when(k == 0)
            def _():
                send_part(my_half * PARTS + PARTS - 1)

            @pl.when(jnp.logical_and(k > 0, near_before))
            def _():
                send_part(other_half * PARTS + k - 1)

            return carry

        lax.fori_loop(0, PARTS, own, 0)
        lax.fori_loop(0, PARTS, others, 0)
        ent_copy = pltpu.make_async_copy(ent_v, ent_out, out_sem)
        ent_copy.start()

        for de in range(1, groups):
            rel_copy(de).wait()
        grel = (grels[0] + grels[1]) + (grels[2] + grels[3])
        new_rel_state = rel_state[...] + jnp.mean(grel * grel, axis=1, keepdims=True)
        rel_now = rel[...] - RATE * (grel / jnp.sqrt(new_rel_state + EPSILON))
        rel_state_out[...] = new_rel_state
        rel_out[...] = rel_now

        @pl.when(near_before)
        def _():
            send_part(other_half * PARTS + PARTS - 1)
    else:
        ent_copy = pltpu.make_async_copy(ent, ent_v, ld_sem.at[0])
        ent_copy.start()
        rel_now = rel[...]
        rel_out[...] = rel_now
        rel_state_out[...] = rel_state[...]
        ent_copy.wait()
    rel3[...] = jnp.concatenate(list(split3(rel_now)) + [jnp.zeros(rel.shape, BF16)], axis=0)

    def rel_of(blk):
        hits = meta[pl.ds(pl.multiple_of(blk * BLOCK, BLOCK), BLOCK), :]
        return hits, split_cols(jnp.dot(hits, rel3[...], preferred_element_type=F32))

    def flat_block(blk):
        return pl.ds(pl.multiple_of(blk * (BLOCK * 4), BLOCK * 4), BLOCK * 4)

    def heads(blk, carry):
        gather_rows(h_ids, blk * BLOCK, BLOCK, ent_v, rows_buf)
        rows = rows_buf[...]
        eh_buf[flat_block(blk), :] = rows
        _, rr = rel_of(blk)
        eh = chunks_of(rows)
        q = [eh[c] * rr[c] - eh[c + 2] * rr[c + 2] for c in (0, 1)]
        q += [eh[c] * rr[c + 2] + eh[c + 2] * rr[c] for c in (0, 1)]
        qb_buf[pl.ds(pl.multiple_of(blk * BLOCK, BLOCK), BLOCK), :] = jnp.concatenate(q, axis=1).astype(BF16)
        return carry

    def widen(source, first, rows):
        def some(g, carry):
            here = pl.ds(pl.multiple_of(first + g * 512, 512), 512)
            table[here, :] = source[here, :].astype(BF16).astype(F32)
            return carry

        lax.fori_loop(0, rows // 512, some, 0)

    if remote:

        def first_half(k, carry):
            heads(k, 0)
            c = my_half * PARTS + k
            copy = table_copy(c, tail, t_relay.at[k], {'data': other_half})
            copy.wait_recv()

            @pl.when(far_after)
            def _():
                copy.start()

            widen(tail, c * part_rows, part_rows)
            return carry

        def second_half(k, carry):
            c = other_half * PARTS + k
            table_copy(c, tail, t_relay.at[k], {'data': other_half}).wait_recv()
            widen(tail, c * part_rows, part_rows)
            return carry

        lax.fori_loop(0, PARTS, first_half, 0)
        send(query_copy, qb_buf, q_send, far_after, after, PARTS, start)
        lax.fori_loop(0, PARTS, second_half, 0)
    else:
        lax.fori_loop(0, count, heads, 0)
        widen(ent_v, 0, table.shape[0])

    for first in range(0, nb.shape[0], BLOCK):
        gather_rows(n_ids, first, BLOCK, table, rows_buf)
        nb[first : first + BLOCK, :] = jnp.concatenate(chunks_of(rows_buf[...]), axis=1).astype(BF16)
    gneg_buf[...] = jnp.zeros_like(gneg_buf)
    grel_out[...] = jnp.zeros_like(grel_out)
    loss_out[...] = jnp.zeros_like(loss_out)

    def gh_copy(blk):
        return pltpu.make_async_copy(eh_buf.at[flat_block(blk)], gh_out.at[flat_block(blk)], gh_sem.at[blk])

    def bucket(blk):
        gather_rows(t_ids, blk * BLOCK, BLOCK, table, rows_buf)
        tb = chunks_of(rows_buf[...])
        qv = qb_buf[pl.ds(pl.multiple_of(blk * BLOCK, BLOCK), BLOCK), :]
        qf = split_cols(qv.astype(F32))
        s = lax.dot_general(qv, nb[...], (((1,), (1,)), ((), ())), preferred_element_type=F32)
        prod = (qf[0] * tb[0] + qf[1] * tb[1]) + (qf[2] * tb[2] + qf[3] * tb[3])
        p = jnp.sum(prod, axis=1, keepdims=True)
        top = jnp.maximum(jnp.max(s, axis=1, keepdims=True), p)
        p_exp = jnp.exp(p - top)
        s_exp = jnp.exp(s - top)
        total = p_exp + jnp.sum(s_exp, axis=1, keepdims=True)
        hits, rr = rel_of(blk)
        w = hits[:, 96:97].astype(F32)
        losses = w * ((top + jnp.log(total)) - p)
        loss_out[...] += jnp.broadcast_to(jnp.sum(losses, keepdims=True), loss_out.shape)
        dp = w * (p_exp / total - 1.0)
        ds = ((w / total) * s_exp).astype(BF16)
        dp_wide = jnp.broadcast_to(dp, (BLOCK, LANES))
        dp_out[blk] = jnp.transpose(dp_wide)[0:1, :]
        gq = split_cols(jnp.dot(ds, nb[...], preferred_element_type=F32))
        gq = [dp_wide * tb[c] + gq[c] for c in range(4)]
        gneg_buf[...] += lax.dot_general(ds, qv, (((0,), (0,)), ((), ())), preferred_element_type=F32)
        e = chunks_of(eh_buf[flat_block(blk), :])
        gr = [gq[c] * e[c] + gq[c + 2] * e[c + 2] for c in (0, 1)]
        gr += [gq[c + 2] * e[c] - gq[c] * e[c + 2] for c in (0, 1)]
        grel = jnp.zeros((LANES, 4 * LANES), F32)
        for piece in split3(jnp.concatenate(gr, axis=1)):
            grel += lax.dot_general(hits, piece, (((0,), (0,)), ((), ())), preferred_element_type=F32)
        grel_out[...] += grel[: grel_out.shape[0], :]
        gh = [gq[c] * rr[c] + gq[c + 2] * rr[c + 2] for c in (0, 1)]
        gh += [gq[c + 2] * rr[c] - gq[c] * rr[c + 2] for c in (0, 1)]
        eh_buf[flat_block(blk), :] = flat_of(gh)
        gh_copy(blk).start()

    def some(k, carry):
        def each(i, carry):
            bucket(k * (count // PARTS) + i)
            return carry

        lax.fori_loop(0, count // PARTS, each, 0)
        if remote:
            c = my_half * PARTS + k
            query_copy(c, qb_in, q_relay.at[k], {'data': other_half}).wait_recv()

            @pl.when(far_before)
            def _():
                query_copy(c, qb_in, q_relay.at[k], {'data': other_half}).start()

        return carry

    if not remote:
        qb_copy = pltpu.make_async_copy(qb_buf, qb_in, gh_sem.at[count])
        qb_copy.start()
    lax.fori_loop(0, PARTS, some, 0)
    if remote:
        dp_copy = pltpu.make_async_remote_copy(dp_out, dp_in, dp_send, dp_recv, device_id={'ent': after}, device_id_type=MESH)
        dp_copy.start()
        send(neg_copy, gneg_buf, n_send, far_after, after, NEG_PARTS, start)
        for k in range(PARTS):
            query_copy(other_half * PARTS + k, qb_in, q_relay.at[k], {'data': other_half}).wait_recv()
        for k in range(NEG_PARTS):
            copy = neg_copy(my_half * NEG_PARTS + k, gneg_in, n_relay.at[k], {'data': other_half})
            copy.wait_recv()
            pl.when(far_before)(copy.start)
        dp_copy.wait()
        ent_copy.wait()
        for blk in range(count):
            gh_copy(blk).wait()
        for k in range(NEG_PARTS):
            neg_copy(other_half * NEG_PARTS + k, gneg_in, n_relay.at[k], {'data': other_half}).wait_recv()
        send(table_copy, tbf, t_send, far_before, before, PARTS, sent)
        send(query_copy, qb_buf, q_send, far_after, after, PARTS, sent)
        send(neg_copy, gneg_buf, n_send, far_after, after, NEG_PARTS, sent)

        @pl.when(far_after)
        def _():
            for k in range(PARTS):
                table_copy(my_half * PARTS + k, tail, t_relay.at[k], {'data': other_half}).wait_send()

        @pl.when(far_before)
        def _():
            for k in range(PARTS):
                query_copy(my_half * PARTS + k, qb_in, q_relay.at[k], {'data': other_half}).wait_send()
            for k in range(NEG_PARTS):
                neg_copy(my_half * NEG_PARTS + k, gneg_in, n_relay.at[k], {'data': other_half}).wait_send()
    else:
        neg_out = pltpu.make_async_copy(gneg_buf, gneg_in, ld_sem.at[0])
        neg_out.start()
        for blk in range(count):
            gh_copy(blk).wait()
        qb_copy.wait()
        neg_out.wait()


def add_rows(k, ids, rows, acc, src):
    id_one, id_two = ids[k], ids[k + 1]
    one, two = row_at(id_one), row_at(id_two)
    first, second = rows[row_at(src), :], rows[row_at(src + 1), :]
    old_one, old_two = acc[one, :], acc[two, :]
    acc[one, :] = old_one + first
    acc[two, :] = old_two + (second + jnp.where(id_one == id_two, first, 0.0))


def scatter_kernel(h_ids, t_ids, n_ids, gneg, gh, dp, qb, acc_out, gt_buf, h_acc, t_acc, *, steps):
    step = pl.program_id(0)

    @pl.when(step == 0)
    def _():
        def clear(g, carry):
            for acc in (h_acc, t_acc):
                acc[pl.ds(pl.multiple_of(g * 256, 256), 256), :] = jnp.zeros((256, LANES), F32)
            return carry

        lax.fori_loop(0, h_acc.shape[0] // 256, clear, 0)

    @pl.when(step < steps)
    def _():
        dp_wide = jnp.transpose(jnp.broadcast_to(dp[0], (LANES, BLOCK)))
        gt_buf[...] = flat_of([c * dp_wide for c in split_cols(qb[...].astype(F32))])

        def some(g, carry):
            base = g * UNROLL
            for u in range(0, UNROLL, 2):
                src = base * 4 + (u // 8) * 32 + u % 8
                k = step * BLOCK + base + u
                add_rows(k, h_ids, gh, h_acc, src)
                add_rows(k, t_ids, gt_buf, t_acc, src)
            return carry

        lax.fori_loop(0, BLOCK // UNROLL, some, 0)

    @pl.when(step >= steps)
    def _():
        @pl.when(step == steps)
        def _():
            half = n_ids.shape[0] // 2

            def some(g, carry):
                base = g * UNROLL
                for u in range(0, UNROLL, 2):
                    src = base * 4 + (u // 8) * 32 + u % 8
                    add_rows(base + u, n_ids, gneg, h_acc, src)
                    add_rows(half + base + u, n_ids, gneg, t_acc, half * 4 + src)
                return carry

            lax.fori_loop(0, half // UNROLL, some, 0)

        rows = acc_out.shape[0]
        here = pl.ds(pl.multiple_of((step - steps) * rows, rows), rows)
        acc_out[...] = h_acc[here, :] + t_acc[here, :]


def final_kernel(acc, ent, state, ent_out, state_out):
    new_rows, new_state = adagrad(ent[...], state[...], acc[...])
    state_out[...] = new_state
    ent_out[...] = new_rows


ANY = pl.BlockSpec(memory_space=pl.ANY)
SMEM = pl.BlockSpec(memory_space=pltpu.SMEM)
VMEM = pl.BlockSpec(memory_space=pltpu.VMEM)


def params(limit):
    return pltpu.CompilerParams(vmem_limit_bytes=limit * MIB, dimension_semantics=("arbitrary",))


def cost(micros):
    return pl.CostEstimate(flops=0, bytes_accessed=int(micros * 3e6), transcendentals=0)


def blocks(shape):
    return pl.BlockSpec(shape, lambda i: (i,) + (0,) * (len(shape) - 1))


def whole(shape):
    return pl.BlockSpec(shape, lambda i: (0,) * len(shape))


def shape_of(shape, dtype=F32):
    return jax.ShapeDtypeStruct(shape, dtype)


def run_round(shift, groups, h_ids, t_ids, n_ids, ent, meta, rel, rel_state, grel, *sums):
    edges, negs, width = h_ids.shape[0], n_ids.shape[0], 4 * LANES
    count = edges // BLOCK
    remote = shift > 0
    dma = pltpu.SemaphoreType.DMA
    out_shape = [
        shape_of((edges * 4, LANES)),
        shape_of((negs, width)),
        shape_of((count, 1, BLOCK)),
        shape_of(rel.shape),
        shape_of((8, LANES)),
        shape_of(rel.shape),
        shape_of(rel_state.shape),
        shape_of((edges, width), BF16),
    ]
    out_specs = [ANY] * 2 + [VMEM] * 5 + [ANY]
    scratch = [
        pltpu.VMEM(ent.shape, F32),
        pltpu.VMEM(ent.shape, F32),
        pltpu.VMEM((edges * 4, LANES), F32),
        pltpu.VMEM((edges, width), BF16),
        pltpu.VMEM((negs, width), BF16),
        pltpu.VMEM((BLOCK * 4, LANES), F32),
        pltpu.VMEM((LANES, width), BF16),
        pltpu.VMEM((negs, width), F32),
        dma((count + 1,)),
        dma((2 * PARTS,)),
    ]
    in_specs = [SMEM] * 3 + [ANY] + [VMEM] * 4
    if remote:
        in_specs += [ANY, VMEM]
        out_shape += [shape_of(ent.shape), shape_of(sums[1].shape)]
        out_specs += [ANY, VMEM]
        scratch += [pltpu.VMEM(ent.shape, BF16)] * 2 + [pltpu.VMEM((groups,) + rel.shape, F32)]
        scratch += [pltpu.VMEM((count, 1, BLOCK), F32), dma((2 * PARTS,)), dma, dma, dma] + [dma((groups - 1,))] * 2
        for parts in (PARTS, PARTS, NEG_PARTS):
            scratch += [dma((2 * parts,)), dma((parts,)), dma((2 * parts,))]
    return pl.pallas_call(
        functools.partial(round_kernel, shift=shift, groups=groups),
        out_shape=out_shape,
        in_specs=in_specs,
        out_specs=out_specs,
        scratch_shapes=scratch,
        compiler_params=pltpu.CompilerParams(
            vmem_limit_bytes=60 * MIB,
            collective_id=shift if remote else None,
            has_side_effects=remote,
        ),
        cost_estimate=cost(60),
        name="round",
    )(h_ids, t_ids, n_ids, ent, meta, rel, rel_state, grel, *sums)


def run_scatter(h_ids, t_ids, n_ids, gneg, gh, dp, qb, flat_rows):
    edges = h_ids.shape[0]
    steps = edges // BLOCK
    out_steps = 8
    out_rows = flat_rows // out_steps
    early = lambda i: jnp.minimum(i, steps - 1)
    late = lambda i: jnp.maximum(i - steps, 0)
    return pl.pallas_call(
        functools.partial(scatter_kernel, steps=steps),
        grid=(steps + out_steps,),
        out_shape=shape_of((flat_rows, LANES)),
        in_specs=[SMEM] * 3
        + [
            VMEM,
            pl.BlockSpec((BLOCK * 4, LANES), lambda i: (early(i), 0)),
            pl.BlockSpec((1, 1, BLOCK), lambda i: (early(i), 0, 0)),
            pl.BlockSpec((BLOCK, 4 * LANES), lambda i: (early(i), 0)),
        ],
        out_specs=pl.BlockSpec((out_rows, LANES), lambda i: (late(i), 0)),
        scratch_shapes=[pltpu.VMEM((BLOCK * 4, LANES), F32)] + [pltpu.VMEM((flat_rows, LANES), F32)] * 2,
        compiler_params=params(60),
        cost_estimate=cost(20),
        name="scatter",
    )(h_ids, t_ids, n_ids, gneg, gh, dp, qb)


def run_final(acc, ent, state):
    steps = 16
    rows = ent.shape[0] // steps
    return pl.pallas_call(
        final_kernel,
        grid=(steps,),
        out_shape=[shape_of(ent.shape), shape_of(state.shape)],
        in_specs=[blocks((rows, LANES)), blocks((rows, LANES)), blocks((rows // 4, 1))],
        out_specs=[blocks((rows, LANES)), blocks((rows // 4, 1))],
        compiler_params=params(60),
        cost_estimate=cost(10),
        name="final",
    )(acc, ent, state)


def solution(mesh):
    groups = mesh.shape['ent']
    row_spec = P(('sweep', 'ent'), None)
    edge_spec = P(('sweep', 'ent'), None, 'data')

    def device_fn(ent_table, ent_state, rel_table, head_idx, tail_idx, rel_idx, edge_mask, neg_idx):
        emb_width = ent_table.shape[1]
        rel_rows = rel_table.shape[0]
        stacked = jnp.stack([head_idx[0], tail_idx[0], rel_idx[0], edge_mask[0]])
        both = lax.all_gather(stacked, 'data')
        both = both.transpose(1, 2, 0, 3).reshape(4, groups, -1)
        bucket_edges = both.shape[2]
        h_flat, t_flat = flat_row(both[0]), flat_row(both[1])
        n_flat = flat_row(neg_idx[0])
        rels, mask = both[2], both[3]
        lane = lax.broadcasted_iota(jnp.int32, (1, 1, LANES), 2)
        hit = ((lane & 31) == rels[:, :, None]) & (lane < 96)
        meta = jnp.where(lane == 96, mask[:, :, None], hit.astype(jnp.int32)).astype(BF16)

        def pairs_of(step, back):
            sign = 1 if back else -1
            return [(i, (i + sign * step) % groups) for i in range(groups)]

        def shift(value, step, back):
            return lax.ppermute(value, 'ent', pairs_of(step, back))

        def group_sum(value):
            for mask in (1, 2):
                value = value + lax.ppermute(value, 'ent', [(i, i ^ mask) for i in range(groups)])
            return value

        in_tails = [t_flat[0]] + [shift(t_flat[s], s, True) for s in range(1, groups)]
        in_negs = [n_flat[0]] + [shift(n_flat[s], s, True) for s in range(1, groups)]

        ent_table, *ids = lax.optimization_barrier((ent_table, *in_tails, *in_negs))
        in_tails, in_negs = ids[:groups], ids[groups:]

        ent = to_flat(ent_table)
        state = ent_state[:, None]
        rel = jnp.pad(rel_table, ((0, 32 - rel_rows), (0, 0)))
        rel_state = jnp.zeros((32, 1), F32)
        grel = jnp.zeros_like(rel)
        losses = []
        sums = ()
        for s in range(groups):
            gh, gneg, dp, grel, loss, rel, rel_state, qb, *new = run_round(
                s, groups, h_flat[s], t_flat[s], n_flat[s], ent, meta[s], rel, rel_state, grel, *sums
            )
            if s > 0:
                ent, state = new
            losses.append(loss[0, 0] / bucket_edges)
            acc = run_scatter(h_flat[s], in_tails[s], in_negs[s], to_flat(gneg), gh, dp, qb, ent.shape[0])
            sums = (acc, state)
        ent, state = run_final(acc, ent, state)
        grel = group_sum(grel)
        rel_state = rel_state + jnp.mean(grel * grel, axis=1, keepdims=True)
        rel = (rel - RATE * (grel / jnp.sqrt(rel_state + EPSILON)))[:rel_rows]
        return from_flat(ent, emb_width // LANES), state[:, 0], rel, jnp.stack(losses)[None, :]

    return jax.shard_map(device_fn, mesh=mesh, in_specs=(row_spec, P(('sweep', 'ent')), P('sweep', None), edge_spec, edge_spec, edge_spec, edge_spec, P(('sweep', 'ent'), None, None)), out_specs=(row_spec, P(('sweep', 'ent')), P('sweep', None), row_spec), check_vma=False)
```

```python
import functools

import jax
import jax.numpy as jnp
from jax import lax
from jax.experimental import pallas as pl
from jax.experimental.pallas import tpu as pltpu
from jax.sharding import PartitionSpec as P

LR_SCALE = 0.2
EPSILON = 1e-8
LANES = 128
BLOCK = 512
UNROLL = 32
PARTS = 8
NEG_PARTS = 4
SUBS = 2
RATE = LR_SCALE * (4 * LANES) ** -0.25
MESH = pl.DeviceIdType.MESH
MIB = 2 ** 20
F32 = jnp.float32
BF16 = jnp.bfloat16


def to_flat(table):
    rows, width = table.shape
    parts = width // LANES
    return table.reshape(rows // 8, 8, parts, LANES).transpose(0, 2, 1, 3).reshape(rows * parts, LANES)


def from_flat(flat, parts):
    rows = flat.shape[0] // parts
    return flat.reshape(rows // 8, parts, 8, LANES).transpose(0, 2, 1, 3).reshape(rows, parts * LANES)


def flat_row(ids):
    return (ids >> 3) * 32 + (ids & 7)


def chunks_of(flat):
    groups = flat.shape[0] // 32
    cube = flat.reshape(groups, 32, LANES)
    return [cube[:, 8 * c : 8 * c + 8, :].reshape(groups * 8, LANES) for c in range(4)]


def flat_of(chunks):
    groups = chunks[0].shape[0] // 8
    cube = jnp.concatenate([c.reshape(groups, 8, LANES) for c in chunks], axis=1)
    return cube.reshape(groups * 32, LANES)


def split_cols(mat):
    return [mat[:, LANES * c : LANES * (c + 1)] for c in range(4)]


def split3(mat):
    hi = mat.astype(BF16)
    rest = mat - hi.astype(F32)
    mid = rest.astype(BF16)
    low = (rest - mid.astype(F32)).astype(BF16)
    return hi, mid, low


def row_at(start):
    return pl.ds(start, 4, stride=8)


def gather_rows(ids, first, count, table, out):
    def some(g, carry):
        base = g * UNROLL
        for u in range(UNROLL):
            out[row_at(base * 4 + (u // 8) * 32 + u % 8), :] = table[row_at(ids[first + base + u]), :]
        return carry

    lax.fori_loop(0, count // UNROLL, some, 0)


def adagrad(ent, state, grad):
    g = chunks_of(grad)
    sq = (g[0] * g[0] + g[1] * g[1]) + (g[2] * g[2] + g[3] * g[3])
    new_state = state + jnp.sum(sq, axis=1, keepdims=True) * (1.0 / (4 * LANES))
    scale = RATE / jnp.sqrt(new_state + EPSILON)
    e = chunks_of(ent)
    return flat_of([e[c] - scale * g[c] for c in range(4)]), new_state


def round_kernel(*refs, shift, groups):
    remote = shift > 0
    h_ids, t_ids, n_ids, ent, meta, rel, rel_state, grel_in, loss_in = refs[:9]
    refs = refs[9:]
    if remote:
        acc, state, refs = refs[0], refs[1], refs[2:]
    gh_out, gneg_in, dp_in, grel_out, loss_out, rel_out, rel_state_out, qb_in = refs[:8]
    refs = refs[8:]
    dp_out = dp_in
    if remote:
        ent_out, state_out, refs = refs[0], refs[1], refs[2:]
    ent_v, table, eh_buf, qb_buf, nb, rows_buf, rel3, gneg_buf, gh_sem, ld_sem = refs[:10]
    refs = refs[10:]
    edges, negs = qb_buf.shape[0], nb.shape[0]
    count = edges // BLOCK
    part_rows = ent_v.shape[0] // (2 * PARTS)

    def part(c):
        return pl.ds(pl.multiple_of(c * part_rows, part_rows), part_rows)

    if remote:
        tail, tbf, grels, dp_out, ac_sem, out_sem, dp_send, dp_recv, g_send, g_recv = refs[:10]
        t_send, t_relay, t_recv, q_send, q_relay, q_recv, n_send, n_relay, n_recv = refs[10:]
        me, my_half = lax.axis_index('ent'), lax.axis_index('data')
        other_half = 1 - my_half
        before, after = lax.rem(me + groups - shift, groups), lax.rem(me + shift, groups)
        far_before = (before // 2) != (me // 2)
        far_after = (after // 2) != (me // 2)
        near_before, near_after = jnp.logical_not(far_before), jnp.logical_not(far_after)

        def loads(c):
            return (
                pltpu.make_async_copy(ent.at[part(c)], ent_v.at[part(c)], ld_sem.at[c]),
                pltpu.make_async_copy(acc.at[part(c)], table.at[part(c)], ac_sem.at[c]),
            )

        for side in (my_half, other_half):
            for k in range(PARTS):
                for copy in loads(side * PARTS + k):
                    copy.start()

        barrier = pltpu.get_barrier_semaphore()
        for dy in range(2):
            for de in range(groups):
                if dy or de:
                    peer = {'data': lax.rem(my_half + dy, 2), 'ent': lax.rem(me + de, groups)}
                    pl.semaphore_signal(barrier, inc=1, device_id=peer, device_id_type=MESH)
        pl.semaphore_wait(barrier, 2 * groups - 1)

        def rel_copy(de):
            return pltpu.make_async_remote_copy(grel_in, grels.at[me], g_send.at[de - 1], g_recv.at[de - 1], device_id={'ent': lax.rem(me + de, groups)}, device_id_type=MESH)

        for de in range(1, groups):
            rel_copy(de).start()
        grels[me] = grel_in[...]

        def piece_copy(source, target, rows, send_sem, recv_sem, c, peer):
            here = pl.ds(pl.multiple_of(c * rows, rows), rows)
            return pltpu.make_async_remote_copy(source.at[here], target.at[here], send_sem, recv_sem.at[c], device_id=peer, device_id_type=MESH)

        def table_copy(c, source, sem, peer):
            return piece_copy(source, tail, part_rows, sem, t_recv, c, peer)

        def query_copy(c, source, sem, peer):
            return piece_copy(source, qb_in, edges // (2 * PARTS), sem, q_recv, c, peer)

        def neg_copy(c, source, sem, peer):
            return piece_copy(source, gneg_in, negs // (2 * NEG_PARTS), sem, n_recv, c, peer)

        def send(copy, source, sems, far, peer, parts, go):
            @pl.when(far)
            def _():
                for k in range(parts):
                    go(copy(my_half * parts + k, source, sems.at[my_half * parts + k], {'ent': peer}))

            @pl.when(jnp.logical_not(far))
            def _():
                for c in range(2 * parts):
                    go(copy(c, source, sems.at[c], {'ent': peer}))

        def start(copy):
            copy.start()

        def sent(copy):
            copy.wait_send()

        def send_part(c):
            table_copy(c, tbf, t_send.at[c], {'ent': before}).start()

        def update(c):
            for copy in loads(c):
                copy.wait()
            rows = pl.ds(pl.multiple_of(c * (part_rows // 4), part_rows // 4), part_rows // 4)
            new_rows, new_state = adagrad(ent_v[part(c), :], state[rows, :], table[part(c), :])
            state_out[rows, :] = new_state
            ent_v[part(c), :] = new_rows
            tbf[part(c), :] = new_rows.astype(BF16)

        def own(k, carry):
            update(my_half * PARTS + k)

            @pl.when(k > 0)
            def _():
                send_part(my_half * PARTS + k - 1)

            return carry

        def others(k, carry):
            update(other_half * PARTS + k)

            @pl.when(k == 0)
            def _():
                send_part(my_half * PARTS + PARTS - 1)

            @pl.when(jnp.logical_and(k > 0, near_before))
            def _():
                send_part(other_half * PARTS + k - 1)

            return carry

        lax.fori_loop(0, PARTS, own, 0)
        lax.fori_loop(0, PARTS, others, 0)
        ent_copy = pltpu.make_async_copy(ent_v, ent_out, out_sem)
        ent_copy.start()

        for de in range(1, groups):
            rel_copy(de).wait()
        grel = (grels[0] + grels[1]) + (grels[2] + grels[3])
        new_rel_state = rel_state[...] + jnp.mean(grel * grel, axis=1, keepdims=True)
        rel_now = rel[...] - RATE * (grel / jnp.sqrt(new_rel_state + EPSILON))
        rel_state_out[...] = new_rel_state
        rel_out[...] = rel_now

        @pl.when(near_before)
        def _():
            send_part(other_half * PARTS + PARTS - 1)
    else:
        ent_copy = pltpu.make_async_copy(ent, ent_v, ld_sem.at[0])
        ent_copy.start()
        rel_now = rel[...]
        rel_out[...] = rel_now
        rel_state_out[...] = rel_state[...]
        ent_copy.wait()
    rel3[...] = jnp.concatenate(list(split3(rel_now)) + [jnp.zeros(rel.shape, BF16)], axis=0)

    def rel_of(blk):
        hits = meta[pl.ds(pl.multiple_of(blk * BLOCK, BLOCK), BLOCK), :]
        return hits, split_cols(jnp.dot(hits, rel3[...], preferred_element_type=F32))

    def flat_block(blk):
        return pl.ds(pl.multiple_of(blk * (BLOCK * 4), BLOCK * 4), BLOCK * 4)

    def heads(blk, carry):
        gather_rows(h_ids, blk * BLOCK, BLOCK, ent_v, rows_buf)
        rows = rows_buf[...]
        eh_buf[flat_block(blk), :] = rows
        _, rr = rel_of(blk)
        eh = chunks_of(rows)
        q = [eh[c] * rr[c] - eh[c + 2] * rr[c + 2] for c in (0, 1)]
        q += [eh[c] * rr[c + 2] + eh[c + 2] * rr[c] for c in (0, 1)]
        qb_buf[pl.ds(pl.multiple_of(blk * BLOCK, BLOCK), BLOCK), :] = jnp.concatenate(q, axis=1).astype(BF16)
        return carry

    def widen(source, first, rows):
        def some(g, carry):
            here = pl.ds(pl.multiple_of(first + g * 512, 512), 512)
            table[here, :] = source[here, :].astype(BF16).astype(F32)
            return carry

        lax.fori_loop(0, rows // 512, some, 0)

    if remote:
        both_ways = shift == groups // 2

        def first_half(k, carry):
            heads(lax.rem(my_half * (count // 2) + k, count), 0)
            if both_ways:
                per = 2 * PARTS // count

                @pl.when(jnp.logical_and(k >= 1, k <= count // 2))
                def _():
                    for i in range(per):
                        c = my_half * PARTS + (k - 1) * per + i
                        query_copy(c, qb_buf, q_send.at[c], {'ent': after}).start()

            c = my_half * PARTS + k
            copy = table_copy(c, tail, t_relay.at[k], {'data': other_half})
            copy.wait_recv()

            @pl.when(far_after)
            def _():
                copy.start()

            widen(tail, c * part_rows, part_rows)
            return carry

        def second_half(k, carry):
            c = other_half * PARTS + k
            table_copy(c, tail, t_relay.at[k], {'data': other_half}).wait_recv()
            widen(tail, c * part_rows, part_rows)
            return carry

        lax.fori_loop(0, PARTS, first_half, 0)
        if not both_ways:
            send(query_copy, qb_buf, q_send, far_after, after, PARTS, start)
        lax.fori_loop(0, PARTS, second_half, 0)
    else:
        lax.fori_loop(0, count, heads, 0)
        widen(ent_v, 0, table.shape[0])

    for first in range(0, nb.shape[0], BLOCK):
        gather_rows(n_ids, first, BLOCK, table, rows_buf)
        nb[first : first + BLOCK, :] = jnp.concatenate(chunks_of(rows_buf[...]), axis=1).astype(BF16)
    gneg_buf[...] = jnp.zeros_like(gneg_buf)
    grel_out[...] = jnp.zeros_like(grel_out)
    loss_out[...] = loss_in[...]
    loss_lane = lax.broadcasted_iota(jnp.int32, loss_out.shape, 1) == shift

    def gh_copy(blk):
        return pltpu.make_async_copy(eh_buf.at[flat_block(blk)], gh_out.at[flat_block(blk)], gh_sem.at[blk])

    def bucket(blk):
        gather_rows(t_ids, blk * BLOCK, BLOCK, table, rows_buf)
        tb = chunks_of(rows_buf[...])
        qv = qb_buf[pl.ds(pl.multiple_of(blk * BLOCK, BLOCK), BLOCK), :]
        qf = split_cols(qv.astype(F32))
        prod = (qf[0] * tb[0] + qf[1] * tb[1]) + (qf[2] * tb[2] + qf[3] * tb[3])
        p = jnp.sum(prod, axis=1, keepdims=True)
        hits, rr = rel_of(blk)
        w = hits[:, 96:97].astype(F32)
        sub = BLOCK // SUBS
        rows = [slice(i * sub, (i + 1) * sub) for i in range(SUBS)]
        s = [lax.dot_general(qv[r], nb[...], (((1,), (1,)), ((), ())), preferred_element_type=F32) for r in rows]
        dps, dss, gqs, losses = [], [], [], []
        for r, sv in zip(rows, s):
            pv, wv = p[r], w[r]
            top = jnp.maximum(jnp.max(sv, axis=1, keepdims=True), pv)
            p_exp = jnp.exp(pv - top)
            s_exp = jnp.exp(sv - top)
            total = p_exp + jnp.sum(s_exp, axis=1, keepdims=True)
            losses.append(wv * ((top + jnp.log(total)) - pv))
            dps.append(wv * (p_exp / total - 1.0))
            dss.append(((wv / total) * s_exp).astype(BF16))
            gqs.append(jnp.dot(dss[-1], nb[...], preferred_element_type=F32))
        loss_sum = jnp.sum(jnp.concatenate(losses, axis=0), keepdims=True)
        loss_out[...] += jnp.where(loss_lane, jnp.broadcast_to(loss_sum, loss_out.shape), 0.0)
        dp_wide = jnp.broadcast_to(jnp.concatenate(dps, axis=0), (BLOCK, LANES))
        dp_out[blk] = jnp.transpose(dp_wide)[0:1, :]
        gq = split_cols(jnp.concatenate(gqs, axis=0))
        gq = [dp_wide * tb[c] + gq[c] for c in range(4)]
        ds = jnp.concatenate(dss, axis=0)
        gneg_buf[...] += lax.dot_general(ds, qv, (((0,), (0,)), ((), ())), preferred_element_type=F32)
        e = chunks_of(eh_buf[flat_block(blk), :])
        gr = [gq[c] * e[c] + gq[c + 2] * e[c + 2] for c in (0, 1)]
        gr += [gq[c + 2] * e[c] - gq[c] * e[c + 2] for c in (0, 1)]
        grel = jnp.zeros((LANES, 4 * LANES), F32)
        for piece in split3(jnp.concatenate(gr, axis=1)):
            grel += lax.dot_general(hits, piece, (((0,), (0,)), ((), ())), preferred_element_type=F32)
        grel_out[...] += grel[: grel_out.shape[0], :]
        gh = [gq[c] * rr[c] + gq[c + 2] * rr[c + 2] for c in (0, 1)]
        gh += [gq[c + 2] * rr[c] - gq[c] * rr[c + 2] for c in (0, 1)]
        eh_buf[flat_block(blk), :] = flat_of(gh)
        gh_copy(blk).start()

    def some(k, carry):
        bucket(k)
        if remote:
            copy = query_copy(my_half * PARTS + k, qb_in, q_relay.at[k], {'data': other_half})
            copy.wait_recv()
            pl.when(far_before)(copy.start)
        return carry

    if not remote:
        qb_copy = pltpu.make_async_copy(qb_buf, qb_in, gh_sem.at[count])
        qb_copy.start()
    lax.fori_loop(0, count, some, 0)
    if remote:
        dp_copy = pltpu.make_async_remote_copy(dp_out, dp_in, dp_send, dp_recv, device_id={'ent': after}, device_id_type=MESH)
        dp_copy.start()
        send(neg_copy, gneg_buf, n_send, far_after, after, NEG_PARTS, start)
        for k in range(PARTS):
            query_copy(other_half * PARTS + k, qb_in, q_relay.at[k], {'data': other_half}).wait_recv()
        for k in range(NEG_PARTS):
            copy = neg_copy(my_half * NEG_PARTS + k, gneg_in, n_relay.at[k], {'data': other_half})
            copy.wait_recv()
            pl.when(far_before)(copy.start)
        dp_copy.wait()
        ent_copy.wait()
        for blk in range(count):
            gh_copy(blk).wait()
        for k in range(NEG_PARTS):
            neg_copy(other_half * NEG_PARTS + k, gneg_in, n_relay.at[k], {'data': other_half}).wait_recv()
        send(table_copy, tbf, t_send, far_before, before, PARTS, sent)
        send(query_copy, qb_buf, q_send, far_after, after, PARTS, sent)
        send(neg_copy, gneg_buf, n_send, far_after, after, NEG_PARTS, sent)

        @pl.when(far_after)
        def _():
            for k in range(PARTS):
                table_copy(my_half * PARTS + k, tail, t_relay.at[k], {'data': other_half}).wait_send()

        @pl.when(far_before)
        def _():
            for k in range(PARTS):
                query_copy(my_half * PARTS + k, qb_in, q_relay.at[k], {'data': other_half}).wait_send()
            for k in range(NEG_PARTS):
                neg_copy(my_half * NEG_PARTS + k, gneg_in, n_relay.at[k], {'data': other_half}).wait_send()
    else:
        neg_out = pltpu.make_async_copy(gneg_buf, gneg_in, ld_sem.at[0])
        neg_out.start()
        for blk in range(count):
            gh_copy(blk).wait()
        qb_copy.wait()
        neg_out.wait()


def add_rows(k, ids, rows, acc, src):
    id_one, id_two = ids[k], ids[k + 1]
    one, two = row_at(id_one), row_at(id_two)
    first, second = rows[row_at(src), :], rows[row_at(src + 1), :]
    old_one, old_two = acc[one, :], acc[two, :]
    acc[one, :] = old_one + first
    acc[two, :] = old_two + (second + jnp.where(id_one == id_two, first, 0.0))


def scatter_kernel(h_ids, t_ids, n_ids, gneg, gh, dp, qb, *refs, steps):
    (ent, state), outs = (refs[:2], refs[2:4]) if len(refs) > 4 else ((None, None), refs[:1])
    gt_buf, h_acc, t_acc = refs[-3:]
    step = pl.program_id(0)
    block = qb.shape[0]

    @pl.when(step == 0)
    def _():
        def clear(g, carry):
            for acc in (h_acc, t_acc):
                acc[pl.ds(pl.multiple_of(g * 256, 256), 256), :] = jnp.zeros((256, LANES), F32)
            return carry

        lax.fori_loop(0, h_acc.shape[0] // 256, clear, 0)

    @pl.when(step < steps)
    def _():
        for i in range(block // BLOCK):
            dp_wide = jnp.transpose(jnp.broadcast_to(dp[i], (LANES, BLOCK)))
            qv = qb[i * BLOCK : (i + 1) * BLOCK, :].astype(F32)
            gt_buf[i * BLOCK * 4 : (i + 1) * BLOCK * 4, :] = flat_of([c * dp_wide for c in split_cols(qv)])

        def some(g, carry):
            base = g * UNROLL
            for u in range(0, UNROLL, 2):
                src = base * 4 + (u // 8) * 32 + u % 8
                k = step * block + base + u
                add_rows(k, h_ids, gh, h_acc, src)
                add_rows(k, t_ids, gt_buf, t_acc, src)
            return carry

        lax.fori_loop(0, block // UNROLL, some, 0)

    @pl.when(step >= steps)
    def _():
        @pl.when(step == steps)
        def _():
            half = n_ids.shape[0] // 2

            def some(g, carry):
                base = g * UNROLL
                for u in range(0, UNROLL, 2):
                    src = base * 4 + (u // 8) * 32 + u % 8
                    add_rows(base + u, n_ids, gneg, h_acc, src)
                    add_rows(half + base + u, n_ids, gneg, t_acc, half * 4 + src)
                return carry

            lax.fori_loop(0, half // UNROLL, some, 0)

        rows = outs[0].shape[0]
        here = pl.ds(pl.multiple_of((step - steps) * rows, rows), rows)
        grad = h_acc[here, :] + t_acc[here, :]
        if ent is None:
            outs[0][...] = grad
        else:
            new_rows, new_state = adagrad(ent[...], state[...], grad)
            outs[0][...] = new_rows
            outs[1][...] = new_state


ANY = pl.BlockSpec(memory_space=pl.ANY)
SMEM = pl.BlockSpec(memory_space=pltpu.SMEM)
VMEM = pl.BlockSpec(memory_space=pltpu.VMEM)


def params(limit):
    return pltpu.CompilerParams(vmem_limit_bytes=limit * MIB, dimension_semantics=("arbitrary",))


def cost(micros):
    return pl.CostEstimate(flops=0, bytes_accessed=int(micros * 3e6), transcendentals=0)


def blocks(shape):
    return pl.BlockSpec(shape, lambda i: (i,) + (0,) * (len(shape) - 1))


def whole(shape):
    return pl.BlockSpec(shape, lambda i: (0,) * len(shape))


def shape_of(shape, dtype=F32):
    return jax.ShapeDtypeStruct(shape, dtype)


def run_round(shift, groups, h_ids, t_ids, n_ids, ent, meta, rel, rel_state, grel, loss, *sums):
    edges, negs, width = h_ids.shape[0], n_ids.shape[0], 4 * LANES
    count = edges // BLOCK
    remote = shift > 0
    dma = pltpu.SemaphoreType.DMA
    out_shape = [
        shape_of((edges * 4, LANES)),
        shape_of((negs, width)),
        shape_of((count, 1, BLOCK)),
        shape_of(rel.shape),
        shape_of((8, LANES)),
        shape_of(rel.shape),
        shape_of(rel_state.shape),
        shape_of((edges, width), BF16),
    ]
    out_specs = [ANY] * 2 + [VMEM] * 5 + [ANY]
    scratch = [
        pltpu.VMEM(ent.shape, F32),
        pltpu.VMEM(ent.shape, F32),
        pltpu.VMEM((edges * 4, LANES), F32),
        pltpu.VMEM((edges, width), BF16),
        pltpu.VMEM((negs, width), BF16),
        pltpu.VMEM((BLOCK * 4, LANES), F32),
        pltpu.VMEM((LANES, width), BF16),
        pltpu.VMEM((negs, width), F32),
        dma((count + 1,)),
        dma((2 * PARTS,)),
    ]
    in_specs = [SMEM] * 3 + [ANY] + [VMEM] * 5
    if remote:
        in_specs += [ANY, VMEM]
        out_shape += [shape_of(ent.shape), shape_of(sums[1].shape)]
        out_specs += [ANY, VMEM]
        scratch += [pltpu.VMEM(ent.shape, BF16)] * 2 + [pltpu.VMEM((groups,) + rel.shape, F32)]
        scratch += [pltpu.VMEM((count, 1, BLOCK), F32), dma((2 * PARTS,)), dma, dma, dma] + [dma((groups - 1,))] * 2
        for parts in (PARTS, PARTS, NEG_PARTS):
            scratch += [dma((2 * parts,)), dma((parts,)), dma((2 * parts,))]
    return pl.pallas_call(
        functools.partial(round_kernel, shift=shift, groups=groups),
        out_shape=out_shape,
        in_specs=in_specs,
        out_specs=out_specs,
        scratch_shapes=scratch,
        compiler_params=pltpu.CompilerParams(
            vmem_limit_bytes=60 * MIB,
            collective_id=shift if remote else None,
            has_side_effects=remote,
        ),
        cost_estimate=cost(60),
        name="round",
    )(h_ids, t_ids, n_ids, ent, meta, rel, rel_state, grel, loss, *sums)


def run_scatter(h_ids, t_ids, n_ids, gneg, gh, dp, qb, flat_rows, *last):
    edges = h_ids.shape[0]
    block = 2 * BLOCK
    steps = edges // block
    out_steps = 4
    out_rows = flat_rows // out_steps
    early = lambda i: jnp.minimum(i, steps - 1)
    late = lambda i: jnp.maximum(i - steps, 0)
    out_specs = [pl.BlockSpec((out_rows, LANES), lambda i: (late(i), 0))]
    out_shape = [shape_of((flat_rows, LANES))]
    if last:
        out_specs.append(pl.BlockSpec((out_rows // 4, 1), lambda i: (late(i), 0)))
        out_shape.append(shape_of((flat_rows // 4, 1)))
    return pl.pallas_call(
        functools.partial(scatter_kernel, steps=steps),
        grid=(steps + out_steps,),
        out_shape=out_shape,
        in_specs=[SMEM] * 3
        + [
            VMEM,
            pl.BlockSpec((block * 4, LANES), lambda i: (early(i), 0)),
            pl.BlockSpec((block // BLOCK, 1, BLOCK), lambda i: (early(i), 0, 0)),
            pl.BlockSpec((block, 4 * LANES), lambda i: (early(i), 0)),
        ]
        + (out_specs if last else []),
        out_specs=out_specs,
        scratch_shapes=[pltpu.VMEM((block * 4, LANES), F32)] + [pltpu.VMEM((flat_rows, LANES), F32)] * 2,
        compiler_params=params(60),
        cost_estimate=cost(20),
        name="scatter",
    )(h_ids, t_ids, n_ids, gneg, gh, dp, qb, *last)


def solution(mesh):
    groups = mesh.shape['ent']
    row_spec = P(('sweep', 'ent'), None)
    edge_spec = P(('sweep', 'ent'), None, 'data')

    def device_fn(ent_table, ent_state, rel_table, head_idx, tail_idx, rel_idx, edge_mask, neg_idx):
        emb_width = ent_table.shape[1]
        rel_rows = rel_table.shape[0]
        stacked = jnp.stack([head_idx[0], tail_idx[0], rel_idx[0], edge_mask[0]])
        both = lax.all_gather(stacked, 'data')
        both = both.transpose(1, 2, 0, 3).reshape(4, groups, -1)
        bucket_edges = both.shape[2]
        h_flat, t_flat = flat_row(both[0]), flat_row(both[1])
        n_flat = flat_row(neg_idx[0])
        rels, mask = both[2], both[3]
        lane = lax.broadcasted_iota(jnp.int32, (1, LANES), 1)

        def meta_of(rels, mask):
            hit = ((lane & 31) == rels[:, None]) & (lane < 96)
            return jnp.where(lane == 96, mask[:, None], hit.astype(jnp.int32)).astype(BF16)

        meta = [meta_of(rels[s], mask[s]) for s in range(groups)]

        def pairs_of(step, back):
            sign = 1 if back else -1
            return [(i, (i + sign * step) % groups) for i in range(groups)]

        def shift(value, step, back):
            return lax.ppermute(value, 'ent', pairs_of(step, back))

        def group_sum(value):
            for mask in (1, 2):
                value = value + lax.ppermute(value, 'ent', [(i, i ^ mask) for i in range(groups)])
            return value

        in_tails = [t_flat[0]] + [shift(t_flat[s], s, True) for s in range(1, groups)]
        in_negs = [n_flat[0]] + [shift(n_flat[s], s, True) for s in range(1, groups)]

        ent = to_flat(ent_table)
        state = ent_state[:, None]
        rel = jnp.pad(rel_table, ((0, 32 - rel_rows), (0, 0)))
        rel_state = jnp.zeros((32, 1), F32)
        grel = jnp.zeros_like(rel)
        loss = jnp.zeros((8, LANES), F32)
        sums = ()
        for s in range(groups):
            gh, gneg, dp, grel, loss, rel, rel_state, qb, *new = run_round(
                s, groups, h_flat[s], t_flat[s], n_flat[s], ent, meta[s], rel, rel_state, grel, loss, *sums
            )
            if s > 0:
                ent, state = new
            last = (ent, state) if s == groups - 1 else ()
            sums = run_scatter(h_flat[s], in_tails[s], in_negs[s], to_flat(gneg), gh, dp, qb, ent.shape[0], *last)
            if s == 0:
                sums, in_tails, in_negs = lax.optimization_barrier((sums, in_tails, in_negs))
            sums = (sums[0], sums[1] if last else state)
        ent, state = sums
        grel = group_sum(grel)
        rel_state = rel_state + jnp.mean(grel * grel, axis=1, keepdims=True)
        rel = (rel - RATE * (grel / jnp.sqrt(rel_state + EPSILON)))[:rel_rows]
        return from_flat(ent, emb_width // LANES), state[:, 0], rel, loss[:1, :groups] / bucket_edges

    return jax.shard_map(device_fn, mesh=mesh, in_specs=(row_spec, P(('sweep', 'ent')), P('sweep', None), edge_spec, edge_spec, edge_spec, edge_spec, P(('sweep', 'ent'), None, None)), out_specs=(row_spec, P(('sweep', 'ent')), P('sweep', None), row_spec), check_vma=False)
```

```python
import functools

import jax
import jax.numpy as jnp
from jax import lax
from jax.experimental import pallas as pl
from jax.experimental.pallas import tpu as pltpu
from jax.sharding import PartitionSpec as P

LR_SCALE = 0.2
EPSILON = 1e-8
LANES = 128
BLOCK = 512
UNROLL = 32
SPREAD = 64
PARTS = 8
NEG_PARTS = 4
RATE = LR_SCALE * (4 * LANES) ** -0.25
MESH = pl.DeviceIdType.MESH
MIB = 2 ** 20
F32 = jnp.float32
BF16 = jnp.bfloat16


def to_flat(table):
    rows, width = table.shape
    parts = width // LANES
    return table.reshape(rows // 8, 8, parts, LANES).transpose(0, 2, 1, 3).reshape(rows * parts, LANES)


def from_flat(flat, parts):
    rows = flat.shape[0] // parts
    return flat.reshape(rows // 8, parts, 8, LANES).transpose(0, 2, 1, 3).reshape(rows, parts * LANES)


def flat_row(ids):
    return (ids >> 3) * 32 + (ids & 7)


def chunks_of(flat):
    groups = flat.shape[0] // 32
    cube = flat.reshape(groups, 32, LANES)
    return [cube[:, 8 * c : 8 * c + 8, :].reshape(groups * 8, LANES) for c in range(4)]


def flat_of(chunks):
    groups = chunks[0].shape[0] // 8
    cube = jnp.concatenate([c.reshape(groups, 8, LANES) for c in chunks], axis=1)
    return cube.reshape(groups * 32, LANES)


def split_cols(mat):
    return [mat[:, LANES * c : LANES * (c + 1)] for c in range(4)]


def split3(mat):
    hi = mat.astype(BF16)
    rest = mat - hi.astype(F32)
    mid = rest.astype(BF16)
    low = (rest - mid.astype(F32)).astype(BF16)
    return hi, mid, low


def row_at(start):
    return pl.ds(start, 4, stride=8)


def gather_rows(ids, first, count, table, out):
    def some(g, carry):
        base = g * UNROLL
        for u in range(UNROLL):
            out[row_at(base * 4 + (u // 8) * 32 + u % 8), :] = table[row_at(ids[first + base + u]), :]
        return carry

    lax.fori_loop(0, count // UNROLL, some, 0)


def adagrad(ent, state, grad):
    g = chunks_of(grad)
    sq = (g[0] * g[0] + g[1] * g[1]) + (g[2] * g[2] + g[3] * g[3])
    new_state = state + jnp.sum(sq, axis=1, keepdims=True) * (1.0 / (4 * LANES))
    scale = RATE / jnp.sqrt(new_state + EPSILON)
    e = chunks_of(ent)
    return flat_of([e[c] - scale * g[c] for c in range(4)]), new_state


def at_once(shift, groups):
    return 1 if shift == groups // 2 else 2


def round_kernel(*refs, shift, groups):
    remote = shift > 0
    blocks_at_once = at_once(shift, groups)
    h_ids, t_ids, n_ids, ent, codes, rel = refs[:6]
    refs = refs[6:]
    if remote:
        rel_state, grel_in, loss_in, acc, state = refs[:5]
        refs = refs[5:]
    gh_out, gneg_in, dp_in, grel_out, loss_out, rel_out, rel_state_out, qb_in = refs[:8]
    refs = refs[8:]
    dp_out = dp_in
    if remote:
        ent_out, state_out, refs = refs[0], refs[1], refs[2:]
    ent_v, table, eh_buf, qb_buf, nb, rows_buf, rel3, gneg_buf, gh_sem, ld_sem = refs[:10]
    refs = refs[10:]
    edges, negs = qb_buf.shape[0], nb.shape[0]
    count = edges // BLOCK
    part_rows = ent_v.shape[0] // (2 * PARTS)

    def part(c):
        return pl.ds(pl.multiple_of(c * part_rows, part_rows), part_rows)

    if remote:
        tail, tbf, grels, dp_out, ac_sem, out_sem, dp_send, dp_recv, g_send, g_recv = refs[:10]
        t_send, t_relay, t_recv, q_send, q_relay, q_recv, n_send, n_relay, n_recv = refs[10:]
        me, my_half = lax.axis_index('ent'), lax.axis_index('data')
        other_half = 1 - my_half
        before, after = lax.rem(me + groups - shift, groups), lax.rem(me + shift, groups)
        far_before = (before // 2) != (me // 2)
        far_after = (after // 2) != (me // 2)
        near_before, near_after = jnp.logical_not(far_before), jnp.logical_not(far_after)

        def loads(c):
            return (
                pltpu.make_async_copy(ent.at[part(c)], ent_v.at[part(c)], ld_sem.at[c]),
                pltpu.make_async_copy(acc.at[part(c)], table.at[part(c)], ac_sem.at[c]),
            )

        for side in (my_half, other_half):
            for k in range(PARTS):
                for copy in loads(side * PARTS + k):
                    copy.start()

        barrier = pltpu.get_barrier_semaphore()
        for dy in range(2):
            for de in range(groups):
                if dy or de:
                    peer = {'data': lax.rem(my_half + dy, 2), 'ent': lax.rem(me + de, groups)}
                    pl.semaphore_signal(barrier, inc=1, device_id=peer, device_id_type=MESH)
        pl.semaphore_wait(barrier, 2 * groups - 1)

        def rel_copy(de):
            return pltpu.make_async_remote_copy(grel_in, grels.at[me], g_send.at[de - 1], g_recv.at[de - 1], device_id={'ent': lax.rem(me + de, groups)}, device_id_type=MESH)

        for de in range(1, groups):
            rel_copy(de).start()
        grels[me] = grel_in[...]

        def piece_copy(source, target, rows, send_sem, recv_sem, c, peer):
            here = pl.ds(pl.multiple_of(c * rows, rows), rows)
            return pltpu.make_async_remote_copy(source.at[here], target.at[here], send_sem, recv_sem.at[c], device_id=peer, device_id_type=MESH)

        def table_copy(c, source, sem, peer):
            return piece_copy(source, tail, part_rows, sem, t_recv, c, peer)

        def query_copy(c, source, sem, peer):
            return piece_copy(source, qb_in, edges // (2 * PARTS), sem, q_recv, c, peer)

        def neg_copy(c, source, sem, peer):
            return piece_copy(source, gneg_in, negs // (2 * NEG_PARTS), sem, n_recv, c, peer)

        def send(copy, source, sems, far, peer, parts, go):
            @pl.when(far)
            def _():
                for k in range(parts):
                    go(copy(my_half * parts + k, source, sems.at[my_half * parts + k], {'ent': peer}))

            @pl.when(jnp.logical_not(far))
            def _():
                for c in range(2 * parts):
                    go(copy(c, source, sems.at[c], {'ent': peer}))

        def start(copy):
            copy.start()

        def sent(copy):
            copy.wait_send()

        def send_part(c):
            table_copy(c, tbf, t_send.at[c], {'ent': before}).start()

        def update(c):
            for copy in loads(c):
                copy.wait()
            rows = pl.ds(pl.multiple_of(c * (part_rows // 4), part_rows // 4), part_rows // 4)
            new_rows, new_state = adagrad(ent_v[part(c), :], state[rows, :], table[part(c), :])
            state_out[rows, :] = new_state
            ent_v[part(c), :] = new_rows
            tbf[part(c), :] = new_rows.astype(BF16)

        def own(k, carry):
            update(my_half * PARTS + k)

            @pl.when(k > 0)
            def _():
                send_part(my_half * PARTS + k - 1)

            return carry

        def others(k, carry):
            update(other_half * PARTS + k)

            @pl.when(k == 0)
            def _():
                send_part(my_half * PARTS + PARTS - 1)

            @pl.when(jnp.logical_and(k > 0, near_before))
            def _():
                send_part(other_half * PARTS + k - 1)

            return carry

        lax.fori_loop(0, PARTS, own, 0)
        lax.fori_loop(0, PARTS, others, 0)
        ent_copy = pltpu.make_async_copy(ent_v, ent_out, out_sem)
        ent_copy.start()

        for de in range(1, groups):
            rel_copy(de).wait()
        grel = (grels[0] + grels[1]) + (grels[2] + grels[3])
        new_rel_state = rel_state[...] + jnp.mean(grel * grel, axis=1, keepdims=True)
        rel_now = rel[...] - RATE * (grel / jnp.sqrt(new_rel_state + EPSILON))
        rel_state_out[...] = new_rel_state
        rel_out[...] = rel_now

        @pl.when(near_before)
        def _():
            send_part(other_half * PARTS + PARTS - 1)
    else:
        ent_copy = pltpu.make_async_copy(ent, ent_v, ld_sem.at[0])
        ent_copy.start()
        rel_now = rel[...]
        rel_out[...] = rel_now
        rel_state_out[...] = jnp.zeros_like(rel_state_out)
        ent_copy.wait()
    rel3[...] = jnp.concatenate(list(split3(rel_now)) + [jnp.zeros(rel.shape, BF16)], axis=0)

    def rel_of(blk):
        row = lax.broadcasted_iota(jnp.int32, (LANES, BLOCK), 0)
        hits = jnp.logical_and((row & 31) == (codes[blk] >> 1), row < 96)
        hits = jnp.where(hits, 1.0, 0.0).astype(BF16)
        return hits, split_cols(lax.dot_general(hits, rel3[...], (((0,), (0,)), ((), ())), preferred_element_type=F32))

    def flat_block(blk):
        return pl.ds(pl.multiple_of(blk * (BLOCK * 4), BLOCK * 4), BLOCK * 4)

    def heads(blk, carry):
        gather_rows(h_ids, blk * BLOCK, BLOCK, ent_v, rows_buf)
        rows = rows_buf[: BLOCK * 4, :]
        eh_buf[flat_block(blk), :] = rows
        _, rr = rel_of(blk)
        eh = chunks_of(rows)
        q = [eh[c] * rr[c] - eh[c + 2] * rr[c + 2] for c in (0, 1)]
        q += [eh[c] * rr[c + 2] + eh[c + 2] * rr[c] for c in (0, 1)]
        qb_buf[pl.ds(pl.multiple_of(blk * BLOCK, BLOCK), BLOCK), :] = jnp.concatenate(q, axis=1).astype(BF16)
        return carry

    def widen(source, first, rows):
        def some(g, carry):
            here = pl.ds(pl.multiple_of(first + g * 512, 512), 512)
            table[here, :] = source[here, :].astype(BF16).astype(F32)
            return carry

        lax.fori_loop(0, rows // 512, some, 0)

    if remote:
        both_ways = shift == groups // 2

        def first_half(k, carry):
            heads(lax.rem(my_half * (count // 2) + k, count), 0)
            if both_ways:
                per = 2 * PARTS // count

                @pl.when(jnp.logical_and(k >= 1, k <= count // 2))
                def _():
                    for i in range(per):
                        c = my_half * PARTS + (k - 1) * per + i
                        query_copy(c, qb_buf, q_send.at[c], {'ent': after}).start()

            c = my_half * PARTS + k
            copy = table_copy(c, tail, t_relay.at[k], {'data': other_half})
            copy.wait_recv()

            @pl.when(far_after)
            def _():
                copy.start()

            widen(tail, c * part_rows, part_rows)
            return carry

        def second_half(k, carry):
            c = other_half * PARTS + k
            table_copy(c, tail, t_relay.at[k], {'data': other_half}).wait_recv()
            widen(tail, c * part_rows, part_rows)
            return carry

        lax.fori_loop(0, PARTS, first_half, 0)
        if not both_ways:
            send(query_copy, qb_buf, q_send, far_after, after, PARTS, start)
        lax.fori_loop(0, PARTS, second_half, 0)
    else:
        lax.fori_loop(0, count, heads, 0)
        widen(ent_v, 0, table.shape[0])

    for first in range(0, nb.shape[0], BLOCK):
        gather_rows(n_ids, first, BLOCK, table, rows_buf)
        nb[first : first + BLOCK, :] = jnp.concatenate(chunks_of(rows_buf[: BLOCK * 4, :]), axis=1).astype(BF16)
    gneg_buf[...] = jnp.zeros_like(gneg_buf)
    grel_out[...] = jnp.zeros_like(grel_out)
    loss_out[...] = loss_in[...] if remote else jnp.zeros_like(loss_out)
    loss_lane = lax.broadcasted_iota(jnp.int32, loss_out.shape, 1) == shift

    wide = blocks_at_once * BLOCK

    def wide_block(blk):
        return pl.ds(pl.multiple_of(blk * (wide * 4), wide * 4), wide * 4)

    def gh_copy(blk):
        return pltpu.make_async_copy(eh_buf.at[wide_block(blk)], gh_out.at[wide_block(blk)], gh_sem.at[blk])

    def bucket(blk):
        gather_rows(t_ids, blk * wide, wide, table, rows_buf)
        tb = chunks_of(rows_buf[...])
        qv = qb_buf[pl.ds(pl.multiple_of(blk * wide, wide), wide), :]
        qf = split_cols(qv.astype(F32))
        prod = (qf[0] * tb[0] + qf[1] * tb[1]) + (qf[2] * tb[2] + qf[3] * tb[3])
        p = jnp.sum(prod, axis=1, keepdims=True)
        found = [rel_of(blk * blocks_at_once + i) for i in range(blocks_at_once)]
        hits = jnp.concatenate([f[0] for f in found], axis=1)
        rr = [jnp.concatenate([f[1][c] for f in found], axis=0) for c in range(4)]
        w = [jnp.transpose(jnp.broadcast_to((codes[blk * blocks_at_once + i] & 1).astype(F32), (LANES, BLOCK)))[:, :1] for i in range(blocks_at_once)]
        w = jnp.concatenate(w, axis=0)
        sub = BLOCK // 2
        rows = [slice(i * sub, (i + 1) * sub) for i in range(wide // sub)]
        s = [lax.dot_general(qv[r], nb[...], (((1,), (1,)), ((), ())), preferred_element_type=F32) for r in rows]
        dps, dss, gqs, losses = [], [], [], []
        for r, sv in zip(rows, s):
            pv, wv = p[r], w[r]
            top = jnp.maximum(jnp.max(sv, axis=1, keepdims=True), pv)
            p_exp = jnp.exp(pv - top)
            s_exp = jnp.exp(sv - top)
            total = p_exp + jnp.sum(s_exp, axis=1, keepdims=True)
            losses.append(wv * ((top + jnp.log(total)) - pv))
            dps.append(wv * (p_exp / total - 1.0))
            dss.append(((wv / total) * s_exp).astype(BF16))
            gqs.append(jnp.dot(dss[-1], nb[...], preferred_element_type=F32))
        loss_sum = jnp.sum(jnp.concatenate(losses, axis=0), keepdims=True)
        loss_out[...] += jnp.where(loss_lane, jnp.broadcast_to(loss_sum, loss_out.shape), 0.0)
        dp_wide = jnp.broadcast_to(jnp.concatenate(dps, axis=0), (wide, LANES))
        for i in range(blocks_at_once):
            dp_out[blk * blocks_at_once + i] = jnp.transpose(dp_wide[i * BLOCK : (i + 1) * BLOCK])[0:1, :]
        gq = split_cols(jnp.concatenate(gqs, axis=0))
        gq = [dp_wide * tb[c] + gq[c] for c in range(4)]
        ds = jnp.concatenate(dss, axis=0)
        gneg_buf[...] += lax.dot_general(ds, qv, (((0,), (0,)), ((), ())), preferred_element_type=F32)
        e = chunks_of(eh_buf[wide_block(blk), :])
        gr = [gq[c] * e[c] + gq[c + 2] * e[c + 2] for c in (0, 1)]
        gr += [gq[c + 2] * e[c] - gq[c] * e[c + 2] for c in (0, 1)]
        grel = jnp.zeros((LANES, 4 * LANES), F32)
        for piece in split3(jnp.concatenate(gr, axis=1)):
            grel += jnp.dot(hits, piece, preferred_element_type=F32)
        grel_out[...] += grel[: grel_out.shape[0], :]
        gh = [gq[c] * rr[c] + gq[c + 2] * rr[c + 2] for c in (0, 1)]
        gh += [gq[c + 2] * rr[c] - gq[c] * rr[c + 2] for c in (0, 1)]
        eh_buf[wide_block(blk), :] = flat_of(gh)
        gh_copy(blk).start()

    def some(k, carry):
        bucket(k)
        if remote:
            for i in range(blocks_at_once):
                copy = query_copy(my_half * PARTS + k * blocks_at_once + i, qb_in, q_relay.at[k * blocks_at_once + i], {'data': other_half})
                copy.wait_recv()
                pl.when(far_before)(copy.start)
        return carry

    if not remote:
        qb_copy = pltpu.make_async_copy(qb_buf, qb_in, gh_sem.at[count])
        qb_copy.start()
    lax.fori_loop(0, count // blocks_at_once, some, 0)
    if remote:
        dp_copy = pltpu.make_async_remote_copy(dp_out, dp_in, dp_send, dp_recv, device_id={'ent': after}, device_id_type=MESH)
        dp_copy.start()
        send(neg_copy, gneg_buf, n_send, far_after, after, NEG_PARTS, start)
        for k in range(PARTS):
            query_copy(other_half * PARTS + k, qb_in, q_relay.at[k], {'data': other_half}).wait_recv()
        for k in range(NEG_PARTS):
            copy = neg_copy(my_half * NEG_PARTS + k, gneg_in, n_relay.at[k], {'data': other_half})
            copy.wait_recv()
            pl.when(far_before)(copy.start)
        dp_copy.wait()
        ent_copy.wait()
        for blk in range(count // blocks_at_once):
            gh_copy(blk).wait()
        for k in range(NEG_PARTS):
            neg_copy(other_half * NEG_PARTS + k, gneg_in, n_relay.at[k], {'data': other_half}).wait_recv()
        send(table_copy, tbf, t_send, far_before, before, PARTS, sent)
        send(query_copy, qb_buf, q_send, far_after, after, PARTS, sent)
        send(neg_copy, gneg_buf, n_send, far_after, after, NEG_PARTS, sent)

        @pl.when(far_after)
        def _():
            for k in range(PARTS):
                table_copy(my_half * PARTS + k, tail, t_relay.at[k], {'data': other_half}).wait_send()

        @pl.when(far_before)
        def _():
            for k in range(PARTS):
                query_copy(my_half * PARTS + k, qb_in, q_relay.at[k], {'data': other_half}).wait_send()
            for k in range(NEG_PARTS):
                neg_copy(my_half * NEG_PARTS + k, gneg_in, n_relay.at[k], {'data': other_half}).wait_send()
    else:
        neg_out = pltpu.make_async_copy(gneg_buf, gneg_in, ld_sem.at[0])
        neg_out.start()
        for blk in range(count // blocks_at_once):
            gh_copy(blk).wait()
        qb_copy.wait()
        neg_out.wait()


def add_rows(k, ids, rows, acc, src):
    id_one, id_two = ids[k], ids[k + 1]
    one, two = row_at(id_one), row_at(id_two)
    first, second = rows[row_at(src), :], rows[row_at(src + 1), :]
    old_one, old_two = acc[one, :], acc[two, :]
    acc[one, :] = old_one + first
    acc[two, :] = old_two + (second + jnp.where(id_one == id_two, first, 0.0))


def scatter_kernel(h_ids, t_ids, n_ids, gneg, gh, dp, qb, *refs, steps):
    (ent, state), outs = (refs[:2], refs[2:4]) if len(refs) > 4 else ((None, None), refs[:1])
    gt_buf, h_acc, t_acc = refs[-3:]
    step = pl.program_id(0)
    block = qb.shape[0]

    @pl.when(step == 0)
    def _():
        def clear(g, carry):
            for acc in (h_acc, t_acc):
                acc[pl.ds(pl.multiple_of(g * 256, 256), 256), :] = jnp.zeros((256, LANES), F32)
            return carry

        lax.fori_loop(0, h_acc.shape[0] // 256, clear, 0)

    @pl.when(step < steps)
    def _():
        for i in range(block // BLOCK):
            dp_wide = jnp.transpose(jnp.broadcast_to(dp[i], (LANES, BLOCK)))
            qv = qb[i * BLOCK : (i + 1) * BLOCK, :].astype(F32)
            gt_buf[i * BLOCK * 4 : (i + 1) * BLOCK * 4, :] = flat_of([c * dp_wide for c in split_cols(qv)])

        def some(g, carry):
            base = g * SPREAD
            for u in range(0, SPREAD, 2):
                src = base * 4 + (u // 8) * 32 + u % 8
                k = step * block + base + u
                add_rows(k, h_ids, gh, h_acc, src)
                add_rows(k, t_ids, gt_buf, t_acc, src)
            return carry

        lax.fori_loop(0, block // SPREAD, some, 0)

    @pl.when(step >= steps)
    def _():
        @pl.when(step == steps)
        def _():
            half = n_ids.shape[0] // 2

            def some(g, carry):
                base = g * SPREAD
                for u in range(0, SPREAD, 2):
                    src = base * 4 + (u // 8) * 32 + u % 8
                    add_rows(base + u, n_ids, gneg, h_acc, src)
                    add_rows(half + base + u, n_ids, gneg, t_acc, half * 4 + src)
                return carry

            lax.fori_loop(0, half // SPREAD, some, 0)

        rows = outs[0].shape[0]
        here = pl.ds(pl.multiple_of((step - steps) * rows, rows), rows)
        grad = h_acc[here, :] + t_acc[here, :]
        if ent is None:
            outs[0][...] = grad
        else:
            new_rows, new_state = adagrad(ent[...], state[...], grad)
            outs[0][...] = new_rows
            outs[1][...] = new_state


ANY = pl.BlockSpec(memory_space=pl.ANY)
SMEM = pl.BlockSpec(memory_space=pltpu.SMEM)
VMEM = pl.BlockSpec(memory_space=pltpu.VMEM)


def params(limit):
    return pltpu.CompilerParams(vmem_limit_bytes=limit * MIB, dimension_semantics=("arbitrary",))


def cost(micros):
    return pl.CostEstimate(flops=0, bytes_accessed=int(micros * 3e6), transcendentals=0)


def blocks(shape):
    return pl.BlockSpec(shape, lambda i: (i,) + (0,) * (len(shape) - 1))


def whole(shape):
    return pl.BlockSpec(shape, lambda i: (0,) * len(shape))


def shape_of(shape, dtype=F32):
    return jax.ShapeDtypeStruct(shape, dtype)


def run_round(shift, groups, h_ids, t_ids, n_ids, ent, codes, rel, *carried):
    edges, negs, width = h_ids.shape[0], n_ids.shape[0], 4 * LANES
    count = edges // BLOCK
    remote = shift > 0
    dma = pltpu.SemaphoreType.DMA
    out_shape = [
        shape_of((edges * 4, LANES)),
        shape_of((negs, width)),
        shape_of((count, 1, BLOCK)),
        shape_of(rel.shape),
        shape_of((8, LANES)),
        shape_of(rel.shape),
        shape_of((rel.shape[0], 1)),
        shape_of((edges, width), BF16),
    ]
    out_specs = [ANY] * 2 + [VMEM] * 5 + [ANY]
    scratch = [
        pltpu.VMEM(ent.shape, F32),
        pltpu.VMEM(ent.shape, F32),
        pltpu.VMEM((edges * 4, LANES), F32),
        pltpu.VMEM((edges, width), BF16),
        pltpu.VMEM((negs, width), BF16),
        pltpu.VMEM((at_once(shift, groups) * BLOCK * 4, LANES), F32),
        pltpu.VMEM((LANES, width), BF16),
        pltpu.VMEM((negs, width), F32),
        dma((count + 1,)),
        dma((2 * PARTS,)),
    ]
    in_specs = [SMEM] * 3 + [ANY] + [VMEM] * 2
    if remote:
        in_specs += [VMEM] * 3 + [ANY, VMEM]
        out_shape += [shape_of(ent.shape), shape_of(carried[-1].shape)]
        out_specs += [ANY, VMEM]
        scratch += [pltpu.VMEM(ent.shape, BF16)] * 2 + [pltpu.VMEM((groups,) + rel.shape, F32)]
        scratch += [pltpu.VMEM((count, 1, BLOCK), F32), dma((2 * PARTS,)), dma, dma, dma] + [dma((groups - 1,))] * 2
        for parts in (PARTS, PARTS, NEG_PARTS):
            scratch += [dma((2 * parts,)), dma((parts,)), dma((2 * parts,))]
    return pl.pallas_call(
        functools.partial(round_kernel, shift=shift, groups=groups),
        out_shape=out_shape,
        in_specs=in_specs,
        out_specs=out_specs,
        scratch_shapes=scratch,
        compiler_params=pltpu.CompilerParams(
            vmem_limit_bytes=60 * MIB,
            collective_id=shift if remote else None,
            has_side_effects=remote,
        ),
        cost_estimate=cost(60),
        name="round",
    )(h_ids, t_ids, n_ids, ent, codes, rel, *carried)


def run_scatter(h_ids, t_ids, n_ids, gneg, gh, dp, qb, flat_rows, *last):
    edges = h_ids.shape[0]
    block = 2 * BLOCK
    steps = edges // block
    out_steps = 4
    out_rows = flat_rows // out_steps
    early = lambda i: jnp.minimum(i, steps - 1)
    late = lambda i: jnp.maximum(i - steps, 0)
    out_specs = [pl.BlockSpec((out_rows, LANES), lambda i: (late(i), 0))]
    out_shape = [shape_of((flat_rows, LANES))]
    if last:
        out_specs.append(pl.BlockSpec((out_rows // 4, 1), lambda i: (late(i), 0)))
        out_shape.append(shape_of((flat_rows // 4, 1)))
    return pl.pallas_call(
        functools.partial(scatter_kernel, steps=steps),
        grid=(steps + out_steps,),
        out_shape=out_shape,
        in_specs=[SMEM] * 3
        + [
            VMEM,
            pl.BlockSpec((block * 4, LANES), lambda i: (early(i), 0)),
            pl.BlockSpec((block // BLOCK, 1, BLOCK), lambda i: (early(i), 0, 0)),
            pl.BlockSpec((block, 4 * LANES), lambda i: (early(i), 0)),
        ]
        + (out_specs if last else []),
        out_specs=out_specs,
        scratch_shapes=[pltpu.VMEM((block * 4, LANES), F32)] + [pltpu.VMEM((flat_rows, LANES), F32)] * 2,
        compiler_params=params(60),
        cost_estimate=cost(20),
        name="scatter",
    )(h_ids, t_ids, n_ids, gneg, gh, dp, qb, *last)


def solution(mesh):
    groups = mesh.shape['ent']
    row_spec = P(('sweep', 'ent'), None)
    edge_spec = P(('sweep', 'ent'), None, 'data')

    def device_fn(ent_table, ent_state, rel_table, head_idx, tail_idx, rel_idx, edge_mask, neg_idx):
        emb_width = ent_table.shape[1]
        rel_rows = rel_table.shape[0]
        stacked = jnp.stack([head_idx[0], tail_idx[0], rel_idx[0], edge_mask[0]])
        both = lax.all_gather(stacked, 'data')
        both = both.transpose(1, 2, 0, 3).reshape(4, groups, -1)
        bucket_edges = both.shape[2]
        h_flat, t_flat = flat_row(both[0]), flat_row(both[1])
        n_flat = flat_row(neg_idx[0])
        rels, mask = both[2], both[3]
        codes = (rels * 2 + mask).reshape(groups, -1, 1, BLOCK)

        def pairs_of(step, back):
            sign = 1 if back else -1
            return [(i, (i + sign * step) % groups) for i in range(groups)]

        def shift(value, step, back):
            return lax.ppermute(value, 'ent', pairs_of(step, back))

        def group_sum(value):
            for mask in (1, 2):
                value = value + lax.ppermute(value, 'ent', [(i, i ^ mask) for i in range(groups)])
            return value

        in_tails = [t_flat[0]] + [shift(t_flat[s], s, True) for s in range(1, groups)]
        in_negs = [n_flat[0]] + [shift(n_flat[s], s, True) for s in range(1, groups)]

        ent = to_flat(ent_table)
        state = ent_state[:, None]
        rel = jnp.pad(rel_table, ((0, 32 - rel_rows), (0, 0)))
        carried = ()
        for s in range(groups):
            gh, gneg, dp, grel, loss, rel, rel_state, qb, *new = run_round(
                s, groups, h_flat[s], t_flat[s], n_flat[s], ent, codes[s], rel, *carried
            )
            if s > 0:
                ent, state = new
            last = (ent, state) if s == groups - 1 else ()
            sums = run_scatter(h_flat[s], in_tails[s], in_negs[s], to_flat(gneg), gh, dp, qb, ent.shape[0], *last)
            if s == 0:
                sums, in_tails, in_negs = lax.optimization_barrier((sums, in_tails, in_negs))
            carried = (rel_state, grel, loss, sums[0], state)
        ent, state = sums
        grel = group_sum(grel)
        rel_state = rel_state + jnp.mean(grel * grel, axis=1, keepdims=True)
        rel = (rel - RATE * (grel / jnp.sqrt(rel_state + EPSILON)))[:rel_rows]
        return from_flat(ent, emb_width // LANES), state[:, 0], rel, loss[:1, :groups] / bucket_edges

    return jax.shard_map(device_fn, mesh=mesh, in_specs=(row_spec, P(('sweep', 'ent')), P('sweep', None), edge_spec, edge_spec, edge_spec, edge_spec, P(('sweep', 'ent'), None, None)), out_specs=(row_spec, P(('sweep', 'ent')), P('sweep', None), row_spec), check_vma=False)
```
